8 devices in a mesh: dp: 1 (over z), tp: 2 (over y), ep: 4 (over x, core).
Axes of the slice: x: 2, y: 2, z: 1, core: 2. Of those that a mesh axis runs over, the one named last changes fastest.
Arguments:
- tokens_x: bfloat16 [3072, 2048], P(('dp', 'ep', 'tp'))
- expert_ids: int32 [3072, 8], P(('dp', 'ep', 'tp'))
- route_gate: float32 [3072, 8], P(('dp', 'ep', 'tp'))
- w_gate: bfloat16 [64, 2048, 1024], P('ep', None, 'tp')
- w_up: bfloat16 [64, 2048, 1024], P('ep', None, 'tp')
- w_down: bfloat16 [64, 1024, 2048], P('ep', 'tp')
Outputs:
- output: bfloat16 [3072, 2048], P(('dp', 'ep', 'tp'))
All inputs are finite; a program needn't handle non-finite values.
Results may differ from the reference program's by a relative error of at most 0.00121.
Values are sent between devices in bfloat16 or wider.
A program may use at most 1 GiB of HBM per device.

```python
import jax
import jax.numpy as jnp
from jax import lax

D_MODEL = 2048
FF_DIM = 1024
EXPERTS = 64
TOP_K = 8
EP_GROUP = 4
TOKENS = 3072


def draw_routing(route_key):
    num_blocks = TOKENS // EXPERTS
    per_dev = EXPERTS // EP_GROUP
    key_pos, key_dev, key_loc = jax.random.split(route_key, 3)
    row_pos = jax.vmap(lambda one_key: jax.random.permutation(one_key, EXPERTS))(jax.random.split(key_pos, num_blocks))
    dev_perm = jax.vmap(lambda one_key: jax.random.permutation(one_key, EP_GROUP))(jax.random.split(key_dev, num_blocks))
    loc_perm = jax.vmap(lambda one_key: jax.random.permutation(one_key, per_dev))(jax.random.split(key_loc, num_blocks * EP_GROUP))
    loc_perm = loc_perm.reshape(num_blocks, EP_GROUP, per_dev)
    slot_offset = jnp.arange(TOP_K, dtype=jnp.int32)

    def block_ids(dev_order, loc_order, positions):
        labels = (positions[:, None] + slot_offset[None, :]) % EXPERTS
        dev_slot = labels % EP_GROUP
        return dev_order[dev_slot] * per_dev + loc_order[dev_slot, labels // EP_GROUP]

    all_ids = jax.vmap(block_ids)(dev_perm, loc_perm, row_pos)
    return all_ids.reshape(TOKENS, TOP_K).astype(jnp.int32)


def setup_inputs(seed: int = 0, part: int = 0) -> dict:
    part_key = jax.random.fold_in(jax.random.key(seed), part)
    key_x, key_gate, key_route = jax.random.split(part_key, 3)
    key_wg, key_wu, key_wd = jax.random.split(jax.random.key(seed + 1), 3)
    tokens_x = jax.random.normal(key_x, (TOKENS, D_MODEL), jnp.float32).astype(jnp.bfloat16)
    expert_ids = draw_routing(key_route)
    route_gate = jax.random.uniform(key_gate, (TOKENS, TOP_K), jnp.float32, 0.5, 1.5) * TOP_K ** -0.5
    w_gate = (jax.random.normal(key_wg, (EXPERTS, D_MODEL, FF_DIM), jnp.float32) * D_MODEL ** -0.5).astype(jnp.bfloat16)
    w_up = (jax.random.normal(key_wu, (EXPERTS, D_MODEL, FF_DIM), jnp.float32) * D_MODEL ** -0.5).astype(jnp.bfloat16)
    w_down = (jax.random.normal(key_wd, (EXPERTS, FF_DIM, D_MODEL), jnp.float32) * FF_DIM ** -0.5).astype(jnp.bfloat16)
    return dict(tokens_x=tokens_x, expert_ids=expert_ids, route_gate=route_gate, w_gate=w_gate, w_up=w_up, w_down=w_down)


def reference(tokens_x, expert_ids, route_gate, w_gate, w_up, w_down):
    expert_cap = TOKENS * TOP_K // EXPERTS
    sort_order = jnp.argsort(expert_ids.reshape(-1), stable=True)
    tok_rows = (sort_order // TOP_K).reshape(EXPERTS, expert_cap)
    gate_rows = route_gate.reshape(-1)[sort_order].reshape(EXPERTS, expert_cap)

    def add_expert(acc_sum, per_expert):
        rows_e, gates_e, wg_e, wu_e, wd_e = per_expert
        x_rows = tokens_x[rows_e]
        h_gate = jnp.dot(x_rows, wg_e, preferred_element_type=jnp.float32)
        h_up = jnp.dot(x_rows, wu_e, preferred_element_type=jnp.float32)
        hidden = (jax.nn.silu(h_gate) * h_up).astype(jnp.bfloat16)
        out_rows = jnp.dot(hidden, wd_e, preferred_element_type=jnp.float32) * gates_e[:, None]
        return acc_sum.at[rows_e].add(out_rows), None

    acc_init = jnp.zeros((TOKENS, D_MODEL), jnp.float32)
    y_total, _ = lax.scan(add_expert, acc_init, (tok_rows, gate_rows, w_gate, w_up, w_down))
    return y_total.astype(jnp.bfloat16)
```

```python
import functools

import jax
import jax.numpy as jnp
from jax import lax
from jax.experimental import pallas as pl
from jax.experimental.pallas import tpu as pltpu
from jax.sharding import PartitionSpec as P

MESH = pl.DeviceIdType.MESH
ROWS = 384
HALF = 192
CAP = 48
DM = 2048
FF = 512
EL = 16
CH = 256
NCH = DM // CH
UNITS = 2 * NCH
WSLOTS = 3


def moe_kernel(rt_ref, x_hbm, wg_hbm, wu_hbm, wd_hbm, y_hbm,
               xa, rtb, key, dt, gp, utri, xdp, hb, wgv, wuv, wdv, ob,
               pm, ps, dr, rf, rs, yv, yst,
               sem_x, sem_w, sem_wd, sem_rs, sem_rr, sem_os, sem_or,
               sem_as, sem_ar, sem_ds, sem_dr, sem_ps, sem_pr, sem_fs, sem_fr,
               sem_ss, sem_sr, sem_ys, sem_yr, sem_out):
    ep = lax.axis_index('ep')
    ty = lax.axis_index('tp')
    cx = ep // 2
    c = ep % 2
    rF = 1 + c
    rS = 2 - c
    my_rows = pl.ds(pl.multiple_of(c * HALF, HALF), HALF)
    other_rows = pl.ds(pl.multiple_of((1 - c) * HALF, HALF), HALF)

    def dev(r, flip):
        nx = 1 - cx if r & 1 else cx
        nc = 1 - c if flip else c
        ny = 1 - ty if r & 2 else ty
        return {'ep': nx * 2 + nc, 'tp': ny}

    partner = dev(0, True)
    dev_f = {'ep': (cx * c + (1 - cx) * (1 - c)) * 2 + c, 'tp': ty * (1 - c) + (1 - ty) * c}
    dev_s = {'ep': (cx * (1 - c) + (1 - cx) * c) * 2 + c, 'tp': ty * c + (1 - ty) * (1 - c)}

    def rcopy(src, dst, ssem, rsem, device):
        return pltpu.make_async_remote_copy(src_ref=src, dst_ref=dst, send_sem=ssem, recv_sem=rsem,
                                            device_id=device, device_id_type=MESH)

    def w_copies(g):
        e = g % EL
        s = g % WSLOTS
        return (pltpu.make_async_copy(wg_hbm.at[e], wgv.at[s], sem_w.at[s, 0]),
                pltpu.make_async_copy(wu_hbm.at[e], wuv.at[s], sem_w.at[s, 1]))

    def wd_copy(u):
        col = pl.ds(pl.multiple_of((u % NCH) * CH, CH), CH)
        return pltpu.make_async_copy(wd_hbm.at[:, :, col], wdv.at[u % 2], sem_wd.at[u % 2])

    def c_f(p):
        return rcopy(xa.at[p, 0, my_rows], xa.at[p, rF, my_rows], sem_as.at[p, 0], sem_ar.at[p, 0], dev_f)

    def c_s(p):
        return rcopy(xa.at[p, 0, my_rows], xa.at[p, rS, my_rows], sem_as.at[p, 1], sem_ar.at[p, 1], dev_s)

    def c_d(p):
        return rcopy(xa.at[p, rF, my_rows], xa.at[p, 3, my_rows], sem_as.at[p, 2], sem_ar.at[p, 2], dev_s)

    def c_pair(p, r):
        return rcopy(xa.at[p, r, my_rows], xa.at[p, r, my_rows], sem_ds.at[p, r], sem_dr.at[p, r], partner)

    own_first = rcopy(xa.at[c, 0, other_rows], xa.at[c, 0, other_rows], sem_os.at[0], sem_or.at[0], partner)
    own_second = rcopy(xa.at[c, 0, my_rows], xa.at[c, 0, my_rows], sem_os.at[1], sem_or.at[1], partner)

    x_load = pltpu.make_async_copy(x_hbm, xa.at[c, 0], sem_x)
    x_load.start()
    for g in range(WSLOTS):
        for cp in w_copies(g):
            cp.start()
    for u in range(2):
        wd_copy(u).start()

    barrier = pltpu.get_barrier_semaphore()
    peers = [(r, flip) for r in range(4) for flip in (False, True) if (r, flip) != (0, False)]
    for r, flip in peers:
        pl.semaphore_signal(barrier, inc=1, device_id=dev(r, flip), device_id_type=MESH)
    pl.semaphore_wait(barrier, len(peers))

    rt_sends = [rcopy(rt_ref, rtb.at[c * 4 + r], sem_rs.at[r, int(flip)], sem_rr.at[c * 4 + r], dev(r, flip))
                for r, flip in peers]
    for cp in rt_sends:
        cp.start()
    x_load.wait()
    own_first.start()
    own_second.start()

    @pl.when(c == 1)
    def _():
        own_first.wait_recv()

    c_f(0).start()
    c_s(0).start()

    rtb[c * 4] = rt_ref[...]
    t_row = lax.broadcasted_iota(jnp.int32, (ROWS, ROWS), 0)
    t_col = lax.broadcasted_iota(jnp.int32, (ROWS, ROWS), 1)
    utri[...] = jnp.where(t_row < t_col, 1.0, 0.0).astype(jnp.bfloat16)
    for r, flip in peers:
        b = (1 - c if flip else c) * 4 + r
        pltpu.make_async_copy(rt_ref, rtb.at[b], sem_rr.at[b]).wait()
    for cp in rt_sends:
        cp.wait_send()

    q_iota = lax.broadcasted_iota(jnp.int32, (CAP, ROWS), 0).astype(jnp.float32)

    def build(b, _):
        p = b // 4
        r = b % 4
        e_iota = (lax.broadcasted_iota(jnp.int32, (EL, ROWS), 0) + ep * EL).astype(jnp.float32)
        chosen = jnp.zeros((EL, ROWS), jnp.float32)
        gate = jnp.zeros((EL, ROWS), jnp.float32)
        for j in range(8):
            hit = rtb[b, j:j + 1, :] == e_iota
            chosen = jnp.where(hit, 1.0, chosen)
            gate = jnp.where(hit, rtb[b, 8 + j:9 + j, :], gate)
        rank = jnp.dot(chosen.astype(jnp.bfloat16), utri[...], preferred_element_type=jnp.float32)
        kk = jnp.where(chosen > 0.0, rank, -1.0)
        key[b] = kk
        hots = []
        for e in range(EL):
            hit = kk[e:e + 1, :] == q_iota
            hots.append(jnp.where(hit, 1.0, 0.0))
            gsum = jnp.sum(jnp.where(hit, gate[e:e + 1, :], 0.0), axis=1, keepdims=True)
            gp[p, e, pl.ds(pl.multiple_of(r * CAP, CAP), CAP), :] = jnp.broadcast_to(gsum, (CAP, 128))
        dt[b] = jnp.concatenate(hots, axis=0).T.astype(jnp.bfloat16)
        return 0

    lax.fori_loop(0, 8, build, 0)

    c_f(0).wait()
    c_d(0).start()
    c_pair(0, rF).start()

    @pl.when(c == 0)
    def _():
        own_first.wait_recv()

    c_f(1).start()
    c_s(1).start()
    c_s(0).wait()
    c_pair(0, rS).start()
    own_first.wait_send()
    own_second.wait()
    c_d(0).wait()
    c_pair(0, 3).start()
    for r in (1, 2, 3):
        c_pair(0, r).wait()

    def pair_step(p, i):
        for r in range(4):
            hots = [jnp.where(key[p * 4 + r, pl.ds(2 * i + j, 1), :] == q_iota, 1.0, 0.0) for j in range(2)]
            hot = jnp.concatenate(hots, axis=0).astype(jnp.bfloat16)
            for n in range(4):
                cols = slice(n * 512, (n + 1) * 512)
                res = jnp.dot(hot, xa[p, r, :, cols], preferred_element_type=jnp.float32).astype(jnp.bfloat16)
                for j in range(2):
                    xdp[j, r * CAP:(r + 1) * CAP, cols] = res[j * CAP:(j + 1) * CAP]
        for j in range(2):
            e = 2 * i + j
            g = p * EL + e
            for cp in w_copies(g):
                cp.wait()
            s = g % WSLOTS
            for n in range(2):
                cols = slice(n * 256, (n + 1) * 256)
                a = jnp.dot(xdp[j], wgv[s, :, cols], preferred_element_type=jnp.float32)
                b = jnp.dot(xdp[j], wuv[s, :, cols], preferred_element_type=jnp.float32)
                hb[p, e, :, cols] = (a * jax.nn.sigmoid(a) * b).astype(jnp.bfloat16)

            @pl.when(g + WSLOTS < 2 * EL)
            def _():
                for cp in w_copies(g + WSLOTS):
                    cp.start()

    def phase0(i, _):
        pair_step(0, i)

        @pl.when(i == 3)
        def _():
            c_f(1).wait()
            c_d(1).start()
            c_pair(1, rF).start()

        @pl.when(i == 5)
        def _():
            c_s(1).wait()
            c_pair(1, rS).start()
        return 0

    lax.fori_loop(0, EL // 2, phase0, 0)

    def k_pair(u):
        s = u % 2
        return rcopy(ps.at[s], dr.at[s], sem_ps.at[s], sem_pr.at[s], partner)

    def k_first(u, which):
        s = u % 3
        src = pm.at[s, 3] if which == 0 else pm.at[s, rF]
        return rcopy(src, rf.at[s, which], sem_fs.at[s, which], sem_fr.at[s, which], dev_f)

    def k_second(u):
        return rcopy(pm.at[u % 3, rS], rs.at[u % 2], sem_ss.at[u % 2], sem_sr.at[u % 2], dev_s)

    def k_out(k):
        cols = pl.ds(pl.multiple_of(k * CH, CH), CH)
        return rcopy(yst.at[:, cols], yv.at[my_rows, cols], sem_ys.at[k], sem_yr.at[k], partner)

    def stage1(u):
        k_pair(u).wait()
        s = u % 3
        for r in (3, 1, 2, 0):
            pm[s, r] = pm[s, r] + dr[u % 2, r]
        k_first(u, 0).start()
        k_first(u, 1).start()

    def stage2(u):
        k_first(u, 0).wait()
        s = u % 3
        pm[s, rS] = pm[s, rS] + rf[s, 0]
        k_second(u).start()

    def stage3(u):
        k_first(u, 1).wait()
        k_second(u).wait()
        s = u % 3
        k = u % NCH
        cols = pl.ds(pl.multiple_of(k * CH, CH), CH)
        tot = (pm[s, 0] + rf[s, 1] + rs[u % 2]).astype(jnp.bfloat16)

        @pl.when(c == u // NCH)
        def _():
            yv[my_rows, cols] = tot

        @pl.when(c != u // NCH)
        def _():
            yst[:, cols] = tot
            k_out(k).start()

    def compute(u):
        p = u // NCH
        s2 = u % 2
        s3 = u % 3
        wd_copy(u).wait()

        def down(e2, _):
            for j in range(2):
                e = 2 * e2 + j
                o = jnp.dot(hb[p, e], wdv[s2, e], preferred_element_type=jnp.float32)
                g = gp[p, e]
                o = o * jnp.concatenate([g, g], axis=1)
                hi = o.astype(jnp.bfloat16)
                rest = o - hi.astype(jnp.float32)
                mid = rest.astype(jnp.bfloat16)
                lo = (rest - mid.astype(jnp.float32)).astype(jnp.bfloat16)
                rows = pl.ds(pl.multiple_of(e * CAP, CAP), CAP)
                for r in range(4):
                    part = slice(r * CAP, (r + 1) * CAP)
                    ob[0, r, rows, :] = hi[part]
                    ob[1, r, rows, :] = mid[part]
                    ob[2, r, rows, :] = lo[part]
            return 0

        lax.fori_loop(0, EL // 2, down, 0)

        @pl.when(u + 2 < UNITS)
        def _():
            wd_copy(u + 2).start()

        def combine(rows, dst, s):
            def body(r, _):
                sel = dt[p * 4 + r, rows, :]
                acc = jnp.dot(sel, ob[0, r], preferred_element_type=jnp.float32)
                acc += jnp.dot(sel, ob[1, r], preferred_element_type=jnp.float32)
                acc += jnp.dot(sel, ob[2, r], preferred_element_type=jnp.float32)
                dst[s, r] = acc
                return 0
            lax.fori_loop(0, 4, body, 0)

        combine(other_rows, ps, s2)
        k_pair(u).start()
        combine(my_rows, pm, s3)

    def unit(i, _):
        @pl.when(i >= 3)
        def _():
            stage3(i - 3)

        @pl.when((i >= 2) & (i < UNITS + 2))
        def _():
            stage2(i - 2)

        @pl.when((i >= 1) & (i < UNITS + 1))
        def _():
            stage1(i - 1)

        @pl.when(i < UNITS)
        def _():
            compute(i)

        @pl.when(i == 0)
        def _():
            c_d(1).wait()
            c_pair(1, 3).start()
            for r in (1, 2, 3):
                c_pair(1, r).wait()

        @pl.when(i < EL // 2)
        def _():
            pair_step(1, i)
        return 0

    lax.fori_loop(0, UNITS + 3, unit, 0)

    for k in range(NCH):
        k_out(k).wait()
    out = pltpu.make_async_copy(yv, y_hbm, sem_out)
    out.start()
    out.wait()


def solution(mesh):
    row_spec = P(('dp', 'ep', 'tp'), None)
    bf, f32 = jnp.bfloat16, jnp.float32

    def local_moe(x, ids, gate, wg, wu, wd):
        rt = jnp.concatenate([ids.T.astype(f32), gate.T], axis=0)
        anyspec = pl.BlockSpec(memory_space=pl.ANY)
        dma = pltpu.SemaphoreType.DMA
        return pl.pallas_call(
            moe_kernel,
            out_shape=jax.ShapeDtypeStruct((ROWS, DM), bf),
            in_specs=[pl.BlockSpec(memory_space=pltpu.VMEM)] + [anyspec] * 4,
            out_specs=anyspec,
            scratch_shapes=[
                pltpu.VMEM((2, 4, ROWS, DM), bf),
                pltpu.VMEM((8, 16, ROWS), f32),
                pltpu.VMEM((8, EL, ROWS), f32),
                pltpu.VMEM((8, ROWS, EL * CAP), bf),
                pltpu.VMEM((2, EL, 4 * CAP, 128), f32),
                pltpu.VMEM((ROWS, ROWS), bf),
                pltpu.VMEM((2, 4 * CAP, DM), bf),
                pltpu.VMEM((2, EL, 4 * CAP, FF), bf),
                pltpu.VMEM((WSLOTS, DM, FF), bf),
                pltpu.VMEM((WSLOTS, DM, FF), bf),
                pltpu.VMEM((2, EL, FF, CH), bf),
                pltpu.VMEM((3, 4, EL * CAP, CH), bf),
                pltpu.VMEM((3, 4, HALF, CH), f32),
                pltpu.VMEM((2, 4, HALF, CH), f32),
                pltpu.VMEM((2, 4, HALF, CH), f32),
                pltpu.VMEM((3, 2, HALF, CH), f32),
                pltpu.VMEM((2, HALF, CH), f32),
                pltpu.VMEM((ROWS, DM), bf),
                pltpu.VMEM((HALF, DM), bf),
                dma, dma((WSLOTS, 2)), dma((2,)), dma((4, 2)), dma((8,)), dma((2,)), dma((2,)),
                dma((2, 3)), dma((2, 3)), dma((2, 4)), dma((2, 4)), dma((2,)), dma((2,)),
                dma((3, 2)), dma((3, 2)), dma((2,)), dma((2,)), dma((NCH,)), dma((NCH,)), dma,
            ],
            compiler_params=pltpu.CompilerParams(
                collective_id=0, has_side_effects=True, vmem_limit_bytes=67_043_328),
        )(rt, x, wg, wu, wd)

    return jax.shard_map(
        local_moe, mesh=mesh,
        in_specs=(row_spec, row_spec, row_spec, P('ep', None, 'tp'), P('ep', None, 'tp'), P('ep', 'tp', None)),
        out_specs=row_spec, check_vma=False)
```

```python
import functools

import jax
import jax.numpy as jnp
from jax import lax
from jax.experimental import pallas as pl
from jax.experimental.pallas import tpu as pltpu
from jax.sharding import PartitionSpec as P

MESH = pl.DeviceIdType.MESH
ROWS = 384
HALF = 192
CAP = 48
DM = 2048
FF = 512
EL = 16
CH = 256
NCH = DM // CH
UNITS = 2 * NCH
WSLOTS = 3


def moe_kernel(rt_ref, x_hbm, wg_hbm, wu_hbm, wd_hbm, y_hbm,
               xa, rtb, key, dt, gp, utri, xdp, hb, wgv, wuv, wdv, ob,
               pm, ps, dr, rf, rs, yv, yst,
               sem_x, sem_w, sem_wd, sem_rs, sem_rr, sem_os, sem_or,
               sem_as, sem_ar, sem_ds, sem_dr, sem_ps, sem_pr, sem_fs, sem_fr,
               sem_ss, sem_sr, sem_ys, sem_yr, sem_out):
    ep = lax.axis_index('ep')
    ty = lax.axis_index('tp')
    cx = ep // 2
    c = ep % 2
    rF = 1 + c
    rS = 2 - c
    my_rows = pl.ds(pl.multiple_of(c * HALF, HALF), HALF)
    other_rows = pl.ds(pl.multiple_of((1 - c) * HALF, HALF), HALF)

    def dev(r, flip):
        nx = 1 - cx if r & 1 else cx
        nc = 1 - c if flip else c
        ny = 1 - ty if r & 2 else ty
        return {'ep': nx * 2 + nc, 'tp': ny}

    partner = dev(0, True)
    dev_f = {'ep': (cx * c + (1 - cx) * (1 - c)) * 2 + c, 'tp': ty * (1 - c) + (1 - ty) * c}
    dev_s = {'ep': (cx * (1 - c) + (1 - cx) * c) * 2 + c, 'tp': ty * c + (1 - ty) * (1 - c)}

    def rcopy(src, dst, ssem, rsem, device):
        return pltpu.make_async_remote_copy(src_ref=src, dst_ref=dst, send_sem=ssem, recv_sem=rsem,
                                            device_id=device, device_id_type=MESH)

    def w_copies(g):
        e = g % EL
        s = g % WSLOTS
        return (pltpu.make_async_copy(wg_hbm.at[e], wgv.at[s], sem_w.at[s, 0]),
                pltpu.make_async_copy(wu_hbm.at[e], wuv.at[s], sem_w.at[s, 1]))

    def wd_copy(u):
        col = pl.ds(pl.multiple_of((u % NCH) * CH, CH), CH)
        return pltpu.make_async_copy(wd_hbm.at[:, :, col], wdv.at[u % 2], sem_wd.at[u % 2])

    def c_f(p):
        return rcopy(xa.at[p, 0, my_rows], xa.at[p, rF, my_rows], sem_as.at[p, 0], sem_ar.at[p, 0], dev_f)

    def c_s(p):
        return rcopy(xa.at[p, 0, my_rows], xa.at[p, rS, my_rows], sem_as.at[p, 1], sem_ar.at[p, 1], dev_s)

    def c_d(p):
        return rcopy(xa.at[p, rF, my_rows], xa.at[p, 3, my_rows], sem_as.at[p, 2], sem_ar.at[p, 2], dev_s)

    def c_pair(p, r):
        return rcopy(xa.at[p, r, my_rows], xa.at[p, r, my_rows], sem_ds.at[p, r], sem_dr.at[p, r], partner)

    own_first = rcopy(xa.at[c, 0, other_rows], xa.at[c, 0, other_rows], sem_os.at[0], sem_or.at[0], partner)
    own_second = rcopy(xa.at[c, 0, my_rows], xa.at[c, 0, my_rows], sem_os.at[1], sem_or.at[1], partner)

    x_load = pltpu.make_async_copy(x_hbm, xa.at[c, 0], sem_x)
    x_load.start()
    for g in range(WSLOTS):
        for cp in w_copies(g):
            cp.start()
    for u in range(2):
        wd_copy(u).start()

    barrier = pltpu.get_barrier_semaphore()
    peers = [(r, flip) for r in range(4) for flip in (False, True) if (r, flip) != (0, False)]
    for r, flip in peers:
        pl.semaphore_signal(barrier, inc=1, device_id=dev(r, flip), device_id_type=MESH)
    pl.semaphore_wait(barrier, len(peers))

    rt_sends = [rcopy(rt_ref, rtb.at[c * 4 + r], sem_rs.at[r, int(flip)], sem_rr.at[c * 4 + r], dev(r, flip))
                for r, flip in peers]
    for cp in rt_sends:
        cp.start()
    x_load.wait()
    own_first.start()
    own_second.start()

    @pl.when(c == 1)
    def _():
        own_first.wait_recv()

    c_f(0).start()
    c_s(0).start()

    rtb[c * 4] = rt_ref[...]
    t_row = lax.broadcasted_iota(jnp.int32, (ROWS, ROWS), 0)
    t_col = lax.broadcasted_iota(jnp.int32, (ROWS, ROWS), 1)
    utri[...] = jnp.where(t_row < t_col, 1.0, 0.0).astype(jnp.bfloat16)
    for r, flip in peers:
        b = (1 - c if flip else c) * 4 + r
        pltpu.make_async_copy(rt_ref, rtb.at[b], sem_rr.at[b]).wait()
    for cp in rt_sends:
        cp.wait_send()

    q_iota = lax.broadcasted_iota(jnp.int32, (CAP, ROWS), 0).astype(jnp.float32)

    def build(b, _):
        p = b // 4
        r = b % 4
        e_iota = (lax.broadcasted_iota(jnp.int32, (EL, ROWS), 0) + ep * EL).astype(jnp.float32)
        chosen = jnp.zeros((EL, ROWS), jnp.float32)
        gate = jnp.zeros((EL, ROWS), jnp.float32)
        for j in range(8):
            hit = rtb[b, j:j + 1, :] == e_iota
            chosen = jnp.where(hit, 1.0, chosen)
            gate = jnp.where(hit, rtb[b, 8 + j:9 + j, :], gate)
        rank = jnp.dot(chosen.astype(jnp.bfloat16), utri[...], preferred_element_type=jnp.float32)
        kk = jnp.where(chosen > 0.0, rank, -1.0)
        key[b] = kk
        hots = []
        for e in range(EL):
            hit = kk[e:e + 1, :] == q_iota
            hots.append(jnp.where(hit, 1.0, 0.0))
            gsum = jnp.sum(jnp.where(hit, gate[e:e + 1, :], 0.0), axis=1, keepdims=True)
            gp[p, e, pl.ds(pl.multiple_of(r * CAP, CAP), CAP), :] = jnp.broadcast_to(gsum, (CAP, 128))
        dt[b] = jnp.concatenate(hots, axis=0).T.astype(jnp.bfloat16)
        return 0

    lax.fori_loop(0, 8, build, 0)

    c_f(0).wait()
    c_d(0).start()
    c_pair(0, rF).start()

    @pl.when(c == 0)
    def _():
        own_first.wait_recv()

    c_s(0).wait()
    c_pair(0, rS).start()
    own_first.wait_send()
    own_second.wait()
    c_d(0).wait()
    c_pair(0, 3).start()
    c_f(1).start()
    c_s(1).start()
    for r in (1, 2, 3):
        c_pair(0, r).wait()

    def dispatch(p, i):
        for r in range(4):
            hots = [jnp.where(key[p * 4 + r, pl.ds(2 * i + j, 1), :] == q_iota, 1.0, 0.0) for j in range(2)]
            hot = jnp.concatenate(hots, axis=0).astype(jnp.bfloat16)
            for n in range(4):
                cols = slice(n * 512, (n + 1) * 512)
                res = jnp.dot(hot, xa[p, r, :, cols], preferred_element_type=jnp.float32).astype(jnp.bfloat16)
                for j in range(2):
                    xdp[j, r * CAP:(r + 1) * CAP, cols] = res[j * CAP:(j + 1) * CAP]

    def experts(p, i):
        for j in range(2):
            e = 2 * i + j
            g = p * EL + e
            for cp in w_copies(g):
                cp.wait()
            s = g % WSLOTS
            for n in range(2):
                cols = slice(n * 256, (n + 1) * 256)
                a = jnp.dot(xdp[j], wgv[s, :, cols], preferred_element_type=jnp.float32)
                b = jnp.dot(xdp[j], wuv[s, :, cols], preferred_element_type=jnp.float32)
                hb[p, e, :, cols] = (a * jax.nn.sigmoid(a) * b).astype(jnp.bfloat16)

            @pl.when(g + WSLOTS < 2 * EL)
            def _():
                for cp in w_copies(g + WSLOTS):
                    cp.start()

    def phase0(i, _):
        dispatch(0, i)
        experts(0, i)

        @pl.when(i == 5)
        def _():
            c_f(1).wait()
            c_d(1).start()
            c_pair(1, rF).start()

        @pl.when(i == 6)
        def _():
            c_s(1).wait()
            c_pair(1, rS).start()
        return 0

    lax.fori_loop(0, EL // 2, phase0, 0)

    def k_pair(u):
        s = u % 2
        return rcopy(ps, dr.at[s], sem_ps, sem_pr.at[s], partner)

    def k_first(u, which):
        s = u % 3
        t = u % 4
        src = pm.at[s, 3] if which == 0 else pm.at[s, rF]
        return rcopy(src, rf.at[t, which], sem_fs.at[t, which], sem_fr.at[t, which], dev_f)

    def k_second(u):
        return rcopy(pm.at[u % 3, rS], rs.at[u % 2], sem_ss.at[u % 2], sem_sr.at[u % 2], dev_s)

    def k_out(k):
        cols = pl.ds(pl.multiple_of(k * CH, CH), CH)
        return rcopy(yst.at[:, cols], yv.at[my_rows, cols], sem_ys.at[k], sem_yr.at[k], partner)

    def stage1(u):
        k_pair(u).wait()
        s = u % 3
        for r in (3, 1, 2, 0):
            pm[s, r] = pm[s, r] + dr[u % 2, r]
        k_first(u, 0).start()
        k_first(u, 1).start()

    def stage2(u):
        k_first(u, 0).wait()
        s = u % 3
        pm[s, rS] = pm[s, rS] + rf[u % 4, 0]
        k_second(u).start()
        k_first(u, 1).wait()
        pm[s, 0] = pm[s, 0] + rf[u % 4, 1]

    def stage3(u):
        k_second(u).wait()
        s = u % 3
        k = u % NCH
        cols = pl.ds(pl.multiple_of(k * CH, CH), CH)
        tot = (pm[s, 0] + rs[u % 2]).astype(jnp.bfloat16)

        @pl.when(c == u // NCH)
        def _():
            yv[my_rows, cols] = tot

        @pl.when(c != u // NCH)
        def _():
            yst[:, cols] = tot
            k_out(k).start()

    def compute(u):
        p = u // NCH
        s2 = u % 2
        s3 = u % 3
        wd_copy(u).wait()

        for e in range(EL):
            o = jnp.dot(hb[p, e], wdv[s2, e], preferred_element_type=jnp.float32)
            g = gp[p, e]
            o = o * jnp.concatenate([g, g], axis=1)
            hi = o.astype(jnp.bfloat16)
            rest = o - hi.astype(jnp.float32)
            mid = rest.astype(jnp.bfloat16)
            lo = (rest - mid.astype(jnp.float32)).astype(jnp.bfloat16)
            rows = slice(e * CAP, (e + 1) * CAP)
            for r in range(4):
                part = slice(r * CAP, (r + 1) * CAP)
                ob[0, r, rows, :] = hi[part]
                ob[1, r, rows, :] = mid[part]
                ob[2, r, rows, :] = lo[part]

        @pl.when(u + 2 < UNITS)
        def _():
            wd_copy(u + 2).start()

        def combine(rows, store):
            for r in range(4):
                sel = dt[p * 4 + r, rows, :]
                acc = jnp.dot(sel, ob[0, r], preferred_element_type=jnp.float32)
                acc += jnp.dot(sel, ob[1, r], preferred_element_type=jnp.float32)
                acc += jnp.dot(sel, ob[2, r], preferred_element_type=jnp.float32)
                store(r, acc)

        def store_other(r, acc):
            ps[r] = acc

        def store_mine(r, acc):
            pm[s3, r] = acc

        combine(other_rows, store_other)
        k_pair(u).start()
        combine(my_rows, store_mine)

    def unit(i, _):
        @pl.when(i >= 3)
        def _():
            stage3(i - 3)

        @pl.when((i >= 2) & (i < UNITS + 2))
        def _():
            stage2(i - 2)

        @pl.when(i < UNITS)
        def _():
            compute(i)

        @pl.when(i == 0)
        def _():
            c_d(1).wait()
            c_pair(1, 3).start()
            for r in (1, 2, 3):
                c_pair(1, r).wait()

        @pl.when(i < EL // 2)
        def _():
            dispatch(1, i)

        @pl.when(i < UNITS)
        def _():
            stage1(i)

        @pl.when(i < EL // 2)
        def _():
            experts(1, i)
        return 0

    lax.fori_loop(0, UNITS + 3, unit, 0)

    for k in range(NCH):
        k_out(k).wait()
    out = pltpu.make_async_copy(yv, y_hbm, sem_out)
    out.start()
    out.wait()


def solution(mesh):
    row_spec = P(('dp', 'ep', 'tp'), None)
    bf, f32 = jnp.bfloat16, jnp.float32

    def local_moe(x, ids, gate, wg, wu, wd):
        rt = jnp.concatenate([ids.T.astype(f32), gate.T], axis=0)
        anyspec = pl.BlockSpec(memory_space=pl.ANY)
        dma = pltpu.SemaphoreType.DMA
        return pl.pallas_call(
            moe_kernel,
            out_shape=jax.ShapeDtypeStruct((ROWS, DM), bf),
            in_specs=[pl.BlockSpec(memory_space=pltpu.VMEM)] + [anyspec] * 4,
            out_specs=anyspec,
            scratch_shapes=[
                pltpu.VMEM((2, 4, ROWS, DM), bf),
                pltpu.VMEM((8, 16, ROWS), f32),
                pltpu.VMEM((8, EL, ROWS), f32),
                pltpu.VMEM((8, ROWS, EL * CAP), bf),
                pltpu.VMEM((2, EL, 4 * CAP, 128), f32),
                pltpu.VMEM((ROWS, ROWS), bf),
                pltpu.VMEM((2, 4 * CAP, DM), bf),
                pltpu.VMEM((2, EL, 4 * CAP, FF), bf),
                pltpu.VMEM((WSLOTS, DM, FF), bf),
                pltpu.VMEM((WSLOTS, DM, FF), bf),
                pltpu.VMEM((2, EL, FF, CH), bf),
                pltpu.VMEM((3, 4, EL * CAP, CH), bf),
                pltpu.VMEM((3, 4, HALF, CH), f32),
                pltpu.VMEM((4, HALF, CH), f32),
                pltpu.VMEM((2, 4, HALF, CH), f32),
                pltpu.VMEM((4, 2, HALF, CH), f32),
                pltpu.VMEM((2, HALF, CH), f32),
                pltpu.VMEM((ROWS, DM), bf),
                pltpu.VMEM((HALF, DM), bf),
                dma, dma((WSLOTS, 2)), dma((2,)), dma((4, 2)), dma((8,)), dma((2,)), dma((2,)),
                dma((2, 3)), dma((2, 3)), dma((2, 4)), dma((2, 4)), dma, dma((2,)),
                dma((4, 2)), dma((4, 2)), dma((2,)), dma((2,)), dma((NCH,)), dma((NCH,)), dma,
            ],
            compiler_params=pltpu.CompilerParams(
                collective_id=0, has_side_effects=True, vmem_limit_bytes=67_043_328),
        )(rt, x, wg, wu, wd)

    return jax.shard_map(
        local_moe, mesh=mesh,
        in_specs=(row_spec, row_spec, row_spec, P('ep', None, 'tp'), P('ep', None, 'tp'), P('ep', 'tp', None)),
        out_specs=row_spec, check_vma=False)
```

```python
import functools

import jax
import jax.numpy as jnp
from jax import lax
from jax.experimental import pallas as pl
from jax.experimental.pallas import tpu as pltpu
from jax.sharding import PartitionSpec as P

MESH = pl.DeviceIdType.MESH
ROWS = 384
HALF = 192
PIECE = 96
CAP = 48
DM = 2048
FF = 512
EL = 16
CH = 256
NCH = DM // CH
UNITS = 2 * NCH
WSLOTS = 3


def moe_kernel(rt_ref, x_hbm, wg_hbm, wu_hbm, wd_hbm, y_hbm,
               xa, rtb, key, dt, gp, utri, xdp, hb, wgv, wuv, wdv, ob,
               pm, ps, dr, rf, rs, yst,
               sem_x, sem_w, sem_wd, sem_rs, sem_rr, sem_os, sem_or,
               sem_as, sem_ar, sem_ds, sem_dr, sem_ps, sem_pr, sem_fs, sem_fr,
               sem_ss, sem_sr, sem_ys, sem_yr, sem_yl):
    ep = lax.axis_index('ep')
    ty = lax.axis_index('tp')
    cx = ep // 2
    c = ep % 2
    rF = 1 + c
    rS = 2 - c
    my_rows = pl.ds(pl.multiple_of(c * HALF, HALF), HALF)
    other_rows = pl.ds(pl.multiple_of((1 - c) * HALF, HALF), HALF)

    def dev(r, flip):
        nx = 1 - cx if r & 1 else cx
        nc = 1 - c if flip else c
        ny = 1 - ty if r & 2 else ty
        return {'ep': nx * 2 + nc, 'tp': ny}

    partner = dev(0, True)
    dev_f = {'ep': (cx * c + (1 - cx) * (1 - c)) * 2 + c, 'tp': ty * (1 - c) + (1 - ty) * c}
    dev_s = {'ep': (cx * (1 - c) + (1 - cx) * c) * 2 + c, 'tp': ty * c + (1 - ty) * (1 - c)}

    def rcopy(src, dst, ssem, rsem, device):
        return pltpu.make_async_remote_copy(src_ref=src, dst_ref=dst, send_sem=ssem, recv_sem=rsem,
                                            device_id=device, device_id_type=MESH)

    def w_copies(g):
        e = g % EL
        s = g % WSLOTS
        return (pltpu.make_async_copy(wg_hbm.at[e], wgv.at[s], sem_w.at[s, 0]),
                pltpu.make_async_copy(wu_hbm.at[e], wuv.at[s], sem_w.at[s, 1]))

    def wd_copy(u):
        col = pl.ds(pl.multiple_of((u % NCH) * CH, CH), CH)
        return pltpu.make_async_copy(wd_hbm.at[:, :, col], wdv.at[u % 2], sem_wd.at[u % 2])

    def piece(q):
        return pl.ds(pl.multiple_of(c * HALF + q * PIECE, PIECE), PIECE)

    def c_f(p, q):
        return rcopy(xa.at[p, 0, piece(q)], xa.at[p, rF, piece(q)], sem_as.at[p, 0, q], sem_ar.at[p, 0, q], dev_f)

    def c_s(p, q):
        return rcopy(xa.at[p, 0, piece(q)], xa.at[p, rS, piece(q)], sem_as.at[p, 1, q], sem_ar.at[p, 1, q], dev_s)

    def c_d(p, q):
        return rcopy(xa.at[p, rF, piece(q)], xa.at[p, 3, piece(q)], sem_as.at[p, 2, q], sem_ar.at[p, 2, q], dev_s)

    def c_pair(p, r, q):
        return rcopy(xa.at[p, r, piece(q)], xa.at[p, r, piece(q)], sem_ds.at[p, r, q], sem_dr.at[p, r, q], partner)

    def rows_first(p, q):
        c_f(p, q).wait()
        c_d(p, q).start()
        c_pair(p, rF, q).start()

    def rows_second(p, q):
        c_s(p, q).wait()
        c_pair(p, rS, q).start()

    def rows_third(p, q):
        c_d(p, q).wait()
        c_pair(p, 3, q).start()

    def rows_done(p, r):
        for q in range(2):
            c_pair(p, r, q).wait()

    own_first = rcopy(xa.at[c, 0, other_rows], xa.at[c, 0, other_rows], sem_os.at[0], sem_or.at[0], partner)
    own_second = rcopy(xa.at[c, 0, my_rows], xa.at[c, 0, my_rows], sem_os.at[1], sem_or.at[1], partner)

    x_load = pltpu.make_async_copy(x_hbm, xa.at[c, 0], sem_x)
    x_load.start()
    for g in range(WSLOTS):
        for cp in w_copies(g):
            cp.start()

    barrier = pltpu.get_barrier_semaphore()
    peers = [(r, flip) for r in range(4) for flip in (False, True) if (r, flip) != (0, False)]
    for r, flip in peers:
        pl.semaphore_signal(barrier, inc=1, device_id=dev(r, flip), device_id_type=MESH)
    pl.semaphore_wait(barrier, len(peers))

    def rt_link(r):
        return rcopy(rt_ref, rtb.at[c * 4 + r], sem_rs.at[r, 0], sem_rr.at[c * 4 + r], dev(r, False))

    def rt_pair(r):
        b = c * 4 + r
        return rcopy(rt_ref if r == 0 else rtb.at[b], rtb.at[b], sem_rs.at[r, 1], sem_rr.at[b], partner)

    for r in (3, 1, 2):
        rt_link(r).start()
    rt_pair(0).start()
    x_load.wait()
    own_first.start()
    own_second.start()

    @pl.when(c == 1)
    def _():
        own_first.wait_recv()

    for q in range(2):
        c_f(0, q).start()
        c_s(0, q).start()

    rtb[c * 4] = rt_ref[...]
    t_row = lax.broadcasted_iota(jnp.int32, (ROWS, ROWS), 0)
    t_col = lax.broadcasted_iota(jnp.int32, (ROWS, ROWS), 1)
    utri[...] = jnp.where(t_row < t_col, 1.0, 0.0).astype(jnp.bfloat16)
    for r in (1, 2, 3):
        rt_link(r).wait()
        rt_pair(r).start()
    for r in range(4):
        rt_pair(r).wait_send()
        b = (1 - c) * 4 + r
        pltpu.make_async_copy(rt_ref, rtb.at[b], sem_rr.at[b]).wait()

    q_iota = lax.broadcasted_iota(jnp.int32, (CAP, ROWS), 0).astype(jnp.float32)

    def build(b, _):
        p = b // 4
        r = b % 4
        e_iota = (lax.broadcasted_iota(jnp.int32, (EL, ROWS), 0) + ep * EL).astype(jnp.float32)
        chosen = jnp.zeros((EL, ROWS), jnp.float32)
        gate = jnp.zeros((EL, ROWS), jnp.float32)
        for j in range(8):
            hit = rtb[b, j:j + 1, :] == e_iota
            chosen = jnp.where(hit, 1.0, chosen)
            gate = jnp.where(hit, rtb[b, 8 + j:9 + j, :], gate)
        rank = jnp.dot(chosen.astype(jnp.bfloat16), utri[...], preferred_element_type=jnp.float32)
        kk = jnp.where(chosen > 0.0, rank, -1.0)
        key[b] = kk
        hots = []
        for e in range(EL):
            hit = kk[e:e + 1, :] == q_iota
            hots.append(jnp.where(hit, 1.0, 0.0))
            gsum = jnp.sum(jnp.where(hit, gate[e:e + 1, :], 0.0), axis=1, keepdims=True)
            gp[p, e, pl.ds(pl.multiple_of(r * CAP, CAP), CAP), :] = jnp.broadcast_to(gsum, (CAP, 128))
        dt[b] = jnp.concatenate(hots, axis=0).T.astype(jnp.bfloat16)
        return 0

    lax.fori_loop(0, 8, build, 0)

    own_first.wait_send()
    own_second.wait()

    @pl.when(c == 0)
    def _():
        own_first.wait_recv()

    def put(e, q, r, val):
        rows = pl.ds(pl.multiple_of(r * CAP, CAP), CAP)
        if e < 8:
            rows = pl.ds(pl.multiple_of((q % 2) * HALF + r * CAP, CAP), CAP)
            wdv[e // 4, (e % 4) * 4 + q // 2, rows, :] = val
        elif e < 14:
            rows = pl.ds(pl.multiple_of((q % 4) * HALF + r * CAP, CAP), CAP)
            ob[(e - 8) * 2 + q // 4, rows, :] = val
        else:
            xdp[e - 14, rows, q * 256:(q + 1) * 256] = val

    def dispatch_block(r, _):
        @pl.when(r == 1)
        def _():
            rows_first(0, 0)
            rows_second(0, 0)
            rows_first(0, 1)
            c_s(1, 0).start()
            c_s(1, 1).start()
            rows_second(0, 1)
            rows_done(0, 1)
            rows_done(0, 2)

        @pl.when(r == 3)
        def _():
            rows_third(0, 0)
            rows_third(0, 1)
            c_f(1, 0).start()
            c_f(1, 1).start()
            rows_done(0, 3)

        kk = key[r]
        for eg in range(4):
            hots = [jnp.where(kk[e:e + 1, :] == q_iota, 1.0, 0.0) for e in range(eg * 4, eg * 4 + 4)]
            hot = jnp.concatenate(hots, axis=0).astype(jnp.bfloat16)
            for n in range(4):
                res = jnp.dot(hot, xa[0, r, :, n * 512:(n + 1) * 512],
                              preferred_element_type=jnp.float32).astype(jnp.bfloat16)
                for j in range(4):
                    for m in range(2):
                        put(eg * 4 + j, n * 2 + m, r, res[j * CAP:(j + 1) * CAP, m * 256:(m + 1) * 256])
        return 0

    lax.fori_loop(0, 4, dispatch_block, 0)

    def expert(p, e, rows_of):
        g = p * EL + e
        for cp in w_copies(g):
            cp.wait()
        s = g % WSLOTS
        xe = rows_of()
        for n in range(2):
            cols = slice(n * 256, (n + 1) * 256)
            a = jnp.dot(xe, wgv[s, :, cols], preferred_element_type=jnp.float32)
            b = jnp.dot(xe, wuv[s, :, cols], preferred_element_type=jnp.float32)
            hb[p, e, :, cols] = (a * jax.nn.sigmoid(a) * b).astype(jnp.bfloat16)

        @pl.when(g + WSLOTS < 2 * EL)
        def _():
            for cp in w_copies(g + WSLOTS):
                cp.start()

    def dispatch(p, i, blocks):
        for r in blocks:
            hots = [jnp.where(key[p * 4 + r, pl.ds(2 * i + j, 1), :] == q_iota, 1.0, 0.0) for j in range(2)]
            hot = jnp.concatenate(hots, axis=0).astype(jnp.bfloat16)
            for n in range(4):
                cols = slice(n * 512, (n + 1) * 512)
                res = jnp.dot(hot, xa[p, r, :, cols], preferred_element_type=jnp.float32).astype(jnp.bfloat16)
                for j in range(2):
                    xdp[j, r * CAP:(r + 1) * CAP, cols] = res[j * CAP:(j + 1) * CAP]

    def experts_a(e, _):
        def rows_of():
            return jnp.concatenate([wdv[e // 4, (e % 4) * 4 + q // 2, (q % 2) * HALF:(q % 2 + 1) * HALF, :]
                                    for q in range(8)], axis=1)
        expert(0, e, rows_of)

        @pl.when(e == 3)
        def _():
            wd_copy(0).start()

        @pl.when(e == 5)
        def _():
            rows_first(1, 0)
            rows_second(1, 0)

        @pl.when(e == 7)
        def _():
            wd_copy(1).start()
        return 0

    def experts_b(e, _):
        def rows_of():
            return jnp.concatenate([ob[(e - 8) * 2 + q // 4, (q % 4) * HALF:(q % 4 + 1) * HALF, :]
                                    for q in range(8)], axis=1)
        expert(0, e, rows_of)
        return 0

    def experts_c(e, _):
        expert(0, e, lambda: xdp[e - 14])
        return 0

    lax.fori_loop(0, 8, experts_a, 0)
    lax.fori_loop(8, 14, experts_b, 0)
    rows_first(1, 1)
    rows_second(1, 1)
    lax.fori_loop(14, 16, experts_c, 0)

    def k_pair(u):
        s = u % 2
        return rcopy(ps, dr.at[s], sem_ps, sem_pr.at[s], partner)

    def k_first(u, which):
        s = u % 3
        t = u % 4
        src = pm.at[s, 3] if which == 0 else pm.at[s, rF]
        return rcopy(src, rf.at[t, which], sem_fs.at[t, which], sem_fr.at[t, which], dev_f)

    def k_second(u):
        return rcopy(pm.at[u % 3, rS], rs.at[u % 2], sem_ss.at[u % 2], sem_sr.at[u % 2], dev_s)

    def k_out(k):
        cols = pl.ds(pl.multiple_of(k * CH, CH), CH)
        return rcopy(yst.at[1, :, cols], y_hbm.at[my_rows, cols], sem_ys.at[k], sem_yr.at[k], partner)

    def k_local(k):
        cols = pl.ds(pl.multiple_of(k * CH, CH), CH)
        return pltpu.make_async_copy(yst.at[0, :, cols], y_hbm.at[my_rows, cols], sem_yl.at[k])

    def stage1(u):
        k_pair(u).wait()
        s = u % 3
        for r in (3, 1, 2, 0):
            pm[s, r] = pm[s, r] + dr[u % 2, r]
        k_first(u, 0).start()
        k_first(u, 1).start()

    def stage2(u):
        k_first(u, 0).wait()
        s = u % 3
        pm[s, rS] = pm[s, rS] + rf[u % 4, 0]
        k_second(u).start()
        k_first(u, 1).wait()
        pm[s, 0] = pm[s, 0] + rf[u % 4, 1]

    def stage3(u):
        k_second(u).wait()
        s = u % 3
        k = u % NCH
        cols = pl.ds(pl.multiple_of(k * CH, CH), CH)
        tot = (pm[s, 0] + rs[u % 2]).astype(jnp.bfloat16)

        @pl.when(c == u // NCH)
        def _():
            yst[0, :, cols] = tot
            k_local(k).start()

        @pl.when(c != u // NCH)
        def _():
            yst[1, :, cols] = tot
            k_out(k).start()

    def compute(u):
        p = u // NCH
        s2 = u % 2
        s3 = u % 3
        wd_copy(u).wait()

        for e in range(EL):
            o = jnp.dot(hb[p, e], wdv[s2, e], preferred_element_type=jnp.float32)
            g = gp[p, e]
            o = o * jnp.concatenate([g, g], axis=1)
            hi = o.astype(jnp.bfloat16)
            rest = o - hi.astype(jnp.float32)
            mid = rest.astype(jnp.bfloat16)
            lo = (rest - mid.astype(jnp.float32)).astype(jnp.bfloat16)
            rows = slice(e * CAP, (e + 1) * CAP)
            for r in range(4):
                part = slice(r * CAP, (r + 1) * CAP)
                ob[r, rows, :] = hi[part]
                ob[4 + r, rows, :] = mid[part]
                ob[8 + r, rows, :] = lo[part]

        @pl.when(u + 2 < UNITS)
        def _():
            wd_copy(u + 2).start()

        def combine(rows, store):
            for r in range(4):
                sel = dt[p * 4 + r, rows, :]
                acc = jnp.dot(sel, ob[r], preferred_element_type=jnp.float32)
                acc += jnp.dot(sel, ob[4 + r], preferred_element_type=jnp.float32)
                acc += jnp.dot(sel, ob[8 + r], preferred_element_type=jnp.float32)
                store(r, acc)

        def store_other(r, acc):
            ps[r] = acc

        def store_mine(r, acc):
            pm[s3, r] = acc

        combine(other_rows, store_other)
        k_pair(u).start()
        combine(my_rows, store_mine)

    def unit(i, _):
        @pl.when(i >= 3)
        def _():
            stage3(i - 3)

        @pl.when((i >= 2) & (i < UNITS + 2))
        def _():
            stage2(i - 2)

        @pl.when(i < UNITS)
        def _():
            compute(i)

        @pl.when(i < EL // 2)
        def _():
            dispatch(1, i, (0, 1, 2))

        @pl.when(i < UNITS)
        def _():
            stage1(i)

        @pl.when(i == 0)
        def _():
            rows_third(1, 0)
            rows_third(1, 1)
            rows_done(1, 3)

        @pl.when(i < EL // 2)
        def _():
            dispatch(1, i, (3,))
            for j in range(2):
                expert(1, 2 * i + j, lambda: xdp[j])
        return 0

    rows_done(1, 1)
    rows_done(1, 2)
    lax.fori_loop(0, UNITS + 3, unit, 0)

    for k in range(NCH):
        k_local(k).wait()
        k_out(k).wait()


def solution(mesh):
    row_spec = P(('dp', 'ep', 'tp'), None)
    bf, f32 = jnp.bfloat16, jnp.float32

    def local_moe(x, ids, gate, wg, wu, wd):
        rt = jnp.concatenate([ids.T.astype(f32), gate.T], axis=0)
        anyspec = pl.BlockSpec(memory_space=pl.ANY)
        dma = pltpu.SemaphoreType.DMA
        return pl.pallas_call(
            moe_kernel,
            out_shape=jax.ShapeDtypeStruct((ROWS, DM), bf),
            in_specs=[pl.BlockSpec(memory_space=pltpu.VMEM)] + [anyspec] * 4,
            out_specs=anyspec,
            scratch_shapes=[
                pltpu.VMEM((2, 4, ROWS, DM), bf),
                pltpu.VMEM((8, 16, ROWS), f32),
                pltpu.VMEM((8, EL, ROWS), f32),
                pltpu.VMEM((8, ROWS, EL * CAP), bf),
                pltpu.VMEM((2, EL, 4 * CAP, 128), f32),
                pltpu.VMEM((ROWS, ROWS), bf),
                pltpu.VMEM((2, 4 * CAP, DM), bf),
                pltpu.VMEM((2, EL, 4 * CAP, FF), bf),
                pltpu.VMEM((WSLOTS, DM, FF), bf),
                pltpu.VMEM((WSLOTS, DM, FF), bf),
                pltpu.VMEM((2, EL, FF, CH), bf),
                pltpu.VMEM((12, EL * CAP, CH), bf),
                pltpu.VMEM((3, 4, HALF, CH), f32),
                pltpu.VMEM((4, HALF, CH), f32),
                pltpu.VMEM((2, 4, HALF, CH), f32),
                pltpu.VMEM((4, 2, HALF, CH), f32),
                pltpu.VMEM((2, HALF, CH), f32),
                pltpu.VMEM((2, HALF, DM), bf),
                dma, dma((WSLOTS, 2)), dma((2,)), dma((4, 2)), dma((8,)), dma((2,)), dma((2,)),
                dma((2, 3, 2)), dma((2, 3, 2)), dma((2, 4, 2)), dma((2, 4, 2)), dma, dma((2,)),
                dma((4, 2)), dma((4, 2)), dma((2,)), dma((2,)), dma((NCH,)), dma((NCH,)), dma((NCH,)),
            ],
            compiler_params=pltpu.CompilerParams(
                collective_id=0, has_side_effects=True, vmem_limit_bytes=67_043_328),
        )(rt, x, wg, wu, wd)

    return jax.shard_map(
        local_moe, mesh=mesh,
        in_specs=(row_spec, row_spec, row_spec, P('ep', None, 'tp'), P('ep', None, 'tp'), P('ep', 'tp', None)),
        out_specs=row_spec, check_vma=False)
```

```python
import functools

import jax
import jax.numpy as jnp
from jax import lax
from jax.experimental import pallas as pl
from jax.experimental.pallas import tpu as pltpu
from jax.sharding import PartitionSpec as P

MESH = pl.DeviceIdType.MESH
ROWS = 384
HALF = 192
PIECE = 96
CAP = 48
DM = 2048
FF = 512
EL = 16
CH = 256
NCH = DM // CH
UNITS = 2 * NCH
WSLOTS = 3
SLOTS = 4


def moe_kernel(ids_ref, gate_ref, x_hbm, wg_hbm, wu_hbm, wd_hbm, y_hbm,
               xa, rtb, key, dt, gp, utri, xdp, hb, wgv, wuv, wdv, ob,
               pm, ps, dr, rf, rs, yst,
               sem_x, sem_w, sem_wd, sem_rs, sem_rr, sem_os, sem_or,
               sem_as, sem_ar, sem_ds, sem_dr, sem_ps, sem_pr, sem_fs, sem_fr,
               sem_ss, sem_sr, sem_ys, sem_yr, sem_yl):
    ep = lax.axis_index('ep')
    ty = lax.axis_index('tp')
    cx = ep // 2
    c = ep % 2
    rF = 1 + c
    rS = 2 - c
    my_rows = pl.ds(pl.multiple_of(c * HALF, HALF), HALF)
    other_rows = pl.ds(pl.multiple_of((1 - c) * HALF, HALF), HALF)

    def dev(r, flip):
        nx = 1 - cx if r & 1 else cx
        nc = 1 - c if flip else c
        ny = 1 - ty if r & 2 else ty
        return {'ep': nx * 2 + nc, 'tp': ny}

    partner = dev(0, True)
    dev_f = {'ep': (cx * c + (1 - cx) * (1 - c)) * 2 + c, 'tp': ty * (1 - c) + (1 - ty) * c}
    dev_s = {'ep': (cx * (1 - c) + (1 - cx) * c) * 2 + c, 'tp': ty * c + (1 - ty) * (1 - c)}

    def rcopy(src, dst, ssem, rsem, device):
        return pltpu.make_async_remote_copy(src_ref=src, dst_ref=dst, send_sem=ssem, recv_sem=rsem,
                                            device_id=device, device_id_type=MESH)

    def w_copies(g):
        e = g % EL
        s = g % WSLOTS
        return (pltpu.make_async_copy(wg_hbm.at[e], wgv.at[s], sem_w.at[s, 0]),
                pltpu.make_async_copy(wu_hbm.at[e], wuv.at[s], sem_w.at[s, 1]))

    def wd_copy(u):
        col = pl.ds(pl.multiple_of((u % NCH) * CH, CH), CH)
        return pltpu.make_async_copy(wd_hbm.at[:, :, col], wdv.at[u % 2], sem_wd.at[u % 2])

    def piece(q):
        return pl.ds(pl.multiple_of(c * HALF + q * PIECE, PIECE), PIECE)

    def c_f(p, q):
        return rcopy(xa.at[p, 0, piece(q)], xa.at[p, rF, piece(q)], sem_as.at[p, 0, q], sem_ar.at[p, 0, q], dev_f)

    def c_s(p, q):
        return rcopy(xa.at[p, 0, piece(q)], xa.at[p, rS, piece(q)], sem_as.at[p, 1, q], sem_ar.at[p, 1, q], dev_s)

    def c_d(p, q):
        return rcopy(xa.at[p, rF, piece(q)], xa.at[p, 3, piece(q)], sem_as.at[p, 2, q], sem_ar.at[p, 2, q], dev_s)

    def c_pair(p, r, q):
        return rcopy(xa.at[p, r, piece(q)], xa.at[p, r, piece(q)], sem_ds.at[p, r, q], sem_dr.at[p, r, q], partner)

    def rows_first(p, q):
        c_f(p, q).wait()
        c_d(p, q).start()
        c_pair(p, rF, q).start()

    def rows_second(p, q):
        c_s(p, q).wait()
        c_pair(p, rS, q).start()

    def rows_third(p, q):
        c_d(p, q).wait()
        c_pair(p, 3, q).start()

    def rows_done(p, r):
        for q in range(2):
            c_pair(p, r, q).wait()

    def own_first(q):
        rows = pl.ds(pl.multiple_of((1 - c) * HALF + q * PIECE, PIECE), PIECE)
        return rcopy(xa.at[c, 0, rows], xa.at[c, 0, rows], sem_os.at[q], sem_or.at[q], partner)

    own_second = rcopy(xa.at[c, 0, my_rows], xa.at[c, 0, my_rows], sem_os.at[2], sem_or.at[2], partner)

    x_load = pltpu.make_async_copy(x_hbm, xa.at[c, 0], sem_x)
    x_load.start()

    rtb[c * 4, 0:8, :] = ids_ref[...].astype(jnp.float32)
    rtb[c * 4, 8:16, :] = gate_ref[...]
    barrier = pltpu.get_barrier_semaphore()
    peers = [(r, flip) for r in range(4) for flip in (False, True) if (r, flip) != (0, False)]
    for r, flip in peers:
        pl.semaphore_signal(barrier, inc=1, device_id=dev(r, flip), device_id_type=MESH)
    pl.semaphore_wait(barrier, len(peers))

    def rt_link(r):
        b = c * 4 + r
        return rcopy(rtb.at[c * 4], rtb.at[b], sem_rs.at[r, 0], sem_rr.at[b], dev(r, False))

    def rt_pair(r):
        b = c * 4 + r
        return rcopy(rtb.at[b], rtb.at[b], sem_rs.at[r, 1], sem_rr.at[b], partner)

    for r in (3, 1, 2):
        rt_link(r).start()
    rt_pair(0).start()
    x_load.wait()
    for q in range(2):
        own_first(q).start()
    for q in range(2):
        @pl.when(c == 1)
        def _():
            own_first(q).wait_recv()

        c_f(0, q).start()
        c_s(0, q).start()
    for q in range(2):
        own_first(q).wait_send()
    own_second.start()
    for g in range(WSLOTS):
        for cp in w_copies(g):
            cp.start()

    t_row = lax.broadcasted_iota(jnp.int32, (ROWS, ROWS), 0)
    t_col = lax.broadcasted_iota(jnp.int32, (ROWS, ROWS), 1)
    utri[...] = jnp.where(t_row < t_col, 1.0, 0.0).astype(jnp.bfloat16)
    for r in (1, 2, 3):
        rt_link(r).wait()
        rt_pair(r).start()
    for r in range(4):
        rt_pair(r).wait_send()
        b = (1 - c) * 4 + r
        pltpu.make_async_copy(rtb.at[b], rtb.at[b], sem_rr.at[b]).wait()

    q_iota = lax.broadcasted_iota(jnp.int32, (CAP, ROWS), 0).astype(jnp.float32)

    def build(b, _):
        p = b // 4
        r = b % 4
        e_iota = (lax.broadcasted_iota(jnp.int32, (EL, ROWS), 0) + ep * EL).astype(jnp.float32)
        chosen = jnp.zeros((EL, ROWS), jnp.float32)
        gate = jnp.zeros((EL, ROWS), jnp.float32)
        for j in range(8):
            hit = rtb[b, j:j + 1, :] == e_iota
            chosen = jnp.where(hit, 1.0, chosen)
            gate = jnp.where(hit, rtb[b, 8 + j:9 + j, :], gate)
        rank = jnp.dot(chosen.astype(jnp.bfloat16), utri[...], preferred_element_type=jnp.float32)
        kk = jnp.where(chosen > 0.0, rank, -1.0)
        key[b] = kk
        hots = []
        for e in range(EL):
            hit = kk[e:e + 1, :] == q_iota
            hots.append(jnp.where(hit, 1.0, 0.0))
            gsum = jnp.sum(jnp.where(hit, gate[e:e + 1, :], 0.0), axis=1, keepdims=True)
            gp[p, e, pl.ds(pl.multiple_of(r * CAP, CAP), CAP), :] = jnp.broadcast_to(gsum, (CAP, 128))
        dt[b] = jnp.concatenate(hots, axis=0).T.astype(jnp.bfloat16)
        return 0

    lax.fori_loop(0, 8, build, 0)

    own_second.wait()

    @pl.when(c == 0)
    def _():
        for q in range(2):
            own_first(q).wait_recv()

    def dispatch_group(r, eg, put):
        kk = key.at[r]
        hots = [jnp.where(kk[pl.ds(eg * 4 + j, 1), :] == q_iota, 1.0, 0.0) for j in range(4)]
        hot = jnp.concatenate(hots, axis=0).astype(jnp.bfloat16)
        for n in range(4):
            res = jnp.dot(hot, xa[0, r, :, n * 512:(n + 1) * 512],
                          preferred_element_type=jnp.float32).astype(jnp.bfloat16)
            for j in range(4):
                for m in range(2):
                    put(j, n * 2 + m, r, res[j * CAP:(j + 1) * CAP, m * 256:(m + 1) * 256])

    def put_wdv(eg):
        def put(j, q, r, val):
            rows = pl.ds(pl.multiple_of((q % 2) * HALF + r * CAP, CAP), CAP)
            wdv[eg, j * 4 + q // 2, rows, :] = val
        return put

    def put_ob(j, q, r, val):
        rows = pl.ds(pl.multiple_of((q % 4) * HALF + r * CAP, CAP), CAP)
        ob[j * 2 + q // 4, rows, :] = val

    def put_xdp(j, q, r, val):
        xdp[j, pl.ds(pl.multiple_of(r * CAP, CAP), CAP), q * 256:(q + 1) * 256] = val

    def dispatch_block(r, _):
        @pl.when(r == 1)
        def _():
            rows_first(0, 0)
            rows_second(0, 0)
            rows_first(0, 1)
            c_s(1, 0).start()
            c_s(1, 1).start()
            rows_second(0, 1)
            rows_done(0, 1)
            rows_done(0, 2)

        for eg in range(2):
            dispatch_group(r, eg, put_wdv(eg))
        dispatch_group(r, 2, put_ob)
        dispatch_group(r, 3, put_xdp)
        return 0

    lax.fori_loop(0, 3, dispatch_block, 0)
    rows_third(0, 0)
    rows_third(0, 1)
    c_f(1, 0).start()
    c_f(1, 1).start()
    rows_done(0, 3)

    def expert(p, e, rows_of):
        g = p * EL + e
        for cp in w_copies(g):
            cp.wait()
        s = g % WSLOTS
        xe = rows_of()
        for n in range(2):
            cols = slice(n * 256, (n + 1) * 256)
            a = jnp.dot(xe, wgv[s, :, cols], preferred_element_type=jnp.float32)
            b = jnp.dot(xe, wuv[s, :, cols], preferred_element_type=jnp.float32)
            hb[p, e, :, cols] = (a * jax.nn.sigmoid(a) * b).astype(jnp.bfloat16)

        @pl.when(e + WSLOTS < EL)
        def _():
            for cp in w_copies(g + WSLOTS):
                cp.start()

    def dispatch(p, quad, blocks):
        for r in blocks:
            hots = [jnp.where(key[p * 4 + r, pl.ds(4 * quad + j, 1), :] == q_iota, 1.0, 0.0) for j in range(4)]
            hot = jnp.concatenate(hots, axis=0).astype(jnp.bfloat16)
            for n in range(4):
                cols = slice(n * 512, (n + 1) * 512)
                res = jnp.dot(hot, xa[p, r, :, cols], preferred_element_type=jnp.float32).astype(jnp.bfloat16)
                for j in range(4):
                    xdp[j, r * CAP:(r + 1) * CAP, cols] = res[j * CAP:(j + 1) * CAP]

    def group_wdv(eg, _):
        dispatch_group(3, eg, put_wdv(eg))

        def one(j, _):
            def rows_of():
                return jnp.concatenate([wdv[eg, j * 4 + q // 2, (q % 2) * HALF:(q % 2 + 1) * HALF, :]
                                        for q in range(8)], axis=1)
            expert(0, eg * 4 + j, rows_of)

            @pl.when((eg == 1) & (j == 1))
            def _():
                rows_first(1, 0)
                rows_second(1, 0)
            return 0

        lax.fori_loop(0, 4, one, 0)
        return 0

    def experts_ob(j, _):
        def rows_of():
            return jnp.concatenate([ob[j * 2 + q // 4, (q % 4) * HALF:(q % 4 + 1) * HALF, :]
                                    for q in range(8)], axis=1)
        expert(0, 8 + j, rows_of)
        return 0

    def experts_xdp(j, _):
        expert(0, 12 + j, lambda: xdp[j])

        @pl.when(j == 0)
        def _():
            rows_first(1, 1)
            rows_second(1, 1)
        return 0

    lax.fori_loop(0, 2, group_wdv, 0)
    wd_copy(0).start()
    dispatch_group(3, 2, put_ob)
    lax.fori_loop(0, 4, experts_ob, 0)
    dispatch_group(3, 3, put_xdp)
    lax.fori_loop(0, 4, experts_xdp, 0)
    for g in range(WSLOTS):
        if g == 2:
            wd_copy(1).start()
        for cp in w_copies(EL + g):
            cp.start()

    def k_pair(u):
        s = u % 2
        return rcopy(ps, dr.at[s], sem_ps, sem_pr.at[s], partner)

    def k_first(u, which):
        s = u % SLOTS
        src = pm.at[s, 3] if which == 0 else pm.at[s, rF]
        return rcopy(src, rf.at[s, which], sem_fs.at[s, which], sem_fr.at[s, which], dev_f)

    def k_second(u):
        s = u % SLOTS
        return rcopy(pm.at[s, rS], rs.at[s], sem_ss.at[s], sem_sr.at[s], dev_s)

    def k_out(u):
        k = u % NCH
        cols = pl.ds(pl.multiple_of(k * CH, CH), CH)
        return rcopy(yst.at[u % SLOTS], y_hbm.at[my_rows, cols], sem_ys.at[k], sem_yr.at[k], partner)

    def k_local(u):
        k = u % NCH
        cols = pl.ds(pl.multiple_of(k * CH, CH), CH)
        return pltpu.make_async_copy(yst.at[u % SLOTS], y_hbm.at[my_rows, cols], sem_yl.at[k])

    def out_drain(u):
        @pl.when(c == u // NCH)
        def _():
            k_local(u).wait()

        @pl.when(c != u // NCH)
        def _():
            k_out(u).wait_send()

    def stage1(u):
        k_pair(u).wait()
        s = u % SLOTS
        for r in (3, 1, 2, 0):
            pm[s, r] = pm[s, r] + dr[u % 2, r]
        k_first(u, 0).start()
        k_first(u, 1).start()

    def stage2(u):
        s = u % SLOTS
        k_first(u, 0).wait()
        pm[s, rS] = pm[s, rS] + rf[s, 0]
        k_second(u).start()
        k_first(u, 1).wait()
        pm[s, 0] = pm[s, 0] + rf[s, 1]

    def stage3(u):
        s = u % SLOTS
        k_second(u).wait()

        @pl.when(u >= SLOTS)
        def _():
            out_drain(u - SLOTS)

        yst[s] = (pm[s, 0] + rs[s]).astype(jnp.bfloat16)

        @pl.when(c == u // NCH)
        def _():
            k_local(u).start()

        @pl.when(c != u // NCH)
        def _():
            k_out(u).start()

    def compute(u):
        p = u // NCH
        s2 = u % 2
        s4 = u % SLOTS
        wd_copy(u).wait()

        for e in range(EL):
            o = jnp.dot(hb[p, e], wdv[s2, e], preferred_element_type=jnp.float32)
            g = gp[p, e]
            o = o * jnp.concatenate([g, g], axis=1)
            hi = o.astype(jnp.bfloat16)
            rest = o - hi.astype(jnp.float32)
            mid = rest.astype(jnp.bfloat16)
            lo = (rest - mid.astype(jnp.float32)).astype(jnp.bfloat16)
            rows = slice(e * CAP, (e + 1) * CAP)
            for r in range(4):
                part = slice(r * CAP, (r + 1) * CAP)
                ob[r, rows, :] = hi[part]
                ob[4 + r, rows, :] = mid[part]
                ob[8 + r, rows, :] = lo[part]

        @pl.when(u + 2 < UNITS)
        def _():
            wd_copy(u + 2).start()

        def combine(rows, store):
            for r in range(4):
                sel = dt[p * 4 + r, rows, :]
                acc = jnp.dot(sel, ob[r], preferred_element_type=jnp.float32)
                acc += jnp.dot(sel, ob[4 + r], preferred_element_type=jnp.float32)
                acc += jnp.dot(sel, ob[8 + r], preferred_element_type=jnp.float32)
                store(r, acc)

        def store_other(r, acc):
            ps[r] = acc

        def store_mine(r, acc):
            pm[s4, r] = acc

        combine(other_rows, store_other)
        k_pair(u).start()
        combine(my_rows, store_mine)

    def unit(i, _):
        @pl.when(i >= 4)
        def _():
            stage3(i - 4)

        @pl.when(i < UNITS)
        def _():
            compute(i)

        def links():
            @pl.when((i >= 2) & (i < UNITS + 2))
            def _():
                stage2(i - 2)

            @pl.when(i < UNITS)
            def _():
                stage1(i)

        @pl.when((i < EL // 2) & (i % 2 == 0))
        def _():
            dispatch(1, i // 2, (0, 1, 2))

        @pl.when(i == 0)
        def _():
            stage1(i)
            rows_third(1, 0)
            rows_third(1, 1)
            rows_done(1, 3)

        @pl.when((i < EL // 2) & (i % 2 == 0))
        def _():
            dispatch(1, i // 2, (3,))

        @pl.when(i < EL // 2)
        def _():
            expert(1, 2 * i, lambda: xdp[(2 * i) % 4])

        @pl.when(i > 0)
        def _():
            links()

        @pl.when(i < EL // 2)
        def _():
            expert(1, 2 * i + 1, lambda: xdp[(2 * i) % 4 + 1])
        return 0

    rows_done(1, 1)
    rows_done(1, 2)
    lax.fori_loop(0, UNITS + 4, unit, 0)

    for u in range(UNITS - SLOTS, UNITS):
        out_drain(u)
    for k in range(NCH):
        k_out(k).wait_recv()


def solution(mesh):
    row_spec = P(('dp', 'ep', 'tp'), None)
    bf, f32 = jnp.bfloat16, jnp.float32

    def local_moe(x, ids, gate, wg, wu, wd):
        anyspec = pl.BlockSpec(memory_space=pl.ANY)
        dma = pltpu.SemaphoreType.DMA
        return pl.pallas_call(
            moe_kernel,
            out_shape=jax.ShapeDtypeStruct((ROWS, DM), bf),
            in_specs=[pl.BlockSpec(memory_space=pltpu.VMEM)] * 2 + [anyspec] * 4,
            out_specs=anyspec,
            scratch_shapes=[
                pltpu.VMEM((2, 4, ROWS, DM), bf),
                pltpu.VMEM((8, 16, ROWS), f32),
                pltpu.VMEM((8, EL, ROWS), f32),
                pltpu.VMEM((8, ROWS, EL * CAP), bf),
                pltpu.VMEM((2, EL, 4 * CAP, 128), f32),
                pltpu.VMEM((ROWS, ROWS), bf),
                pltpu.VMEM((4, 4 * CAP, DM), bf),
                pltpu.VMEM((2, EL, 4 * CAP, FF), bf),
                pltpu.VMEM((WSLOTS, DM, FF), bf),
                pltpu.VMEM((WSLOTS, DM, FF), bf),
                pltpu.VMEM((2, EL, FF, CH), bf),
                pltpu.VMEM((12, EL * CAP, CH), bf),
                pltpu.VMEM((SLOTS, 4, HALF, CH), f32),
                pltpu.VMEM((4, HALF, CH), f32),
                pltpu.VMEM((2, 4, HALF, CH), f32),
                pltpu.VMEM((SLOTS, 2, HALF, CH), f32),
                pltpu.VMEM((SLOTS, HALF, CH), f32),
                pltpu.VMEM((SLOTS, HALF, CH), bf),
                dma, dma((WSLOTS, 2)), dma((2,)), dma((4, 2)), dma((8,)), dma((3,)), dma((3,)),
                dma((2, 3, 2)), dma((2, 3, 2)), dma((2, 4, 2)), dma((2, 4, 2)), dma, dma((2,)),
                dma((SLOTS, 2)), dma((SLOTS, 2)), dma((SLOTS,)), dma((SLOTS,)), dma((NCH,)), dma((NCH,)), dma((NCH,)),
            ],
            compiler_params=pltpu.CompilerParams(
                collective_id=0, has_side_effects=True, vmem_limit_bytes=67_043_328),
        )(ids.T, gate.T, x, wg, wu, wd)

    return jax.shard_map(
        local_moe, mesh=mesh,
        in_specs=(row_spec, row_spec, row_spec, P('ep', None, 'tp'), P('ep', None, 'tp'), P('ep', 'tp', None)),
        out_specs=row_spec, check_vma=False)
```

```python
import functools

import jax
import jax.numpy as jnp
from jax import lax
from jax.experimental import pallas as pl
from jax.experimental.pallas import tpu as pltpu
from jax.sharding import PartitionSpec as P

MESH = pl.DeviceIdType.MESH
ROWS = 384
HALF = 192
PIECE = 96
CAP = 48
DM = 2048
FF = 512
EL = 16
CH = 256
NCH = DM // CH
UNITS = 2 * NCH
WSLOTS = 3
SLOTS = 4


def moe_kernel(ids_ref, gate_ref, x_hbm, wg_hbm, wu_hbm, wd_hbm, y_hbm,
               xa, rtb, key, dt, gp, utri, xdp, hb, wgv, wuv, wdv, ob,
               pm, ps, dr, rf, rs, yst,
               sem_x, sem_w, sem_wd, sem_rs, sem_rr, sem_os, sem_or,
               sem_as, sem_ar, sem_ds, sem_dr, sem_ps, sem_pr, sem_fs, sem_fr,
               sem_ss, sem_sr, sem_ys, sem_yr, sem_yl):
    ep = lax.axis_index('ep')
    ty = lax.axis_index('tp')
    cx = ep // 2
    c = ep % 2
    rF = 1 + c
    rS = 2 - c
    my_rows = pl.ds(pl.multiple_of(c * HALF, HALF), HALF)
    other_rows = pl.ds(pl.multiple_of((1 - c) * HALF, HALF), HALF)

    def dev(r, flip):
        nx = 1 - cx if r & 1 else cx
        nc = 1 - c if flip else c
        ny = 1 - ty if r & 2 else ty
        return {'ep': nx * 2 + nc, 'tp': ny}

    partner = dev(0, True)
    dev_f = {'ep': (cx * c + (1 - cx) * (1 - c)) * 2 + c, 'tp': ty * (1 - c) + (1 - ty) * c}
    dev_s = {'ep': (cx * (1 - c) + (1 - cx) * c) * 2 + c, 'tp': ty * c + (1 - ty) * (1 - c)}

    def rcopy(src, dst, ssem, rsem, device):
        return pltpu.make_async_remote_copy(src_ref=src, dst_ref=dst, send_sem=ssem, recv_sem=rsem,
                                            device_id=device, device_id_type=MESH)

    def w_copies(g):
        e = g % EL
        s = g % WSLOTS
        return (pltpu.make_async_copy(wg_hbm.at[e], wgv.at[s], sem_w.at[s, 0]),
                pltpu.make_async_copy(wu_hbm.at[e], wuv.at[s], sem_w.at[s, 1]))

    def wd_copy(u):
        col = pl.ds(pl.multiple_of((u % NCH) * CH, CH), CH)
        return pltpu.make_async_copy(wd_hbm.at[:, :, col], wdv.at[u % 2], sem_wd.at[u % 2])

    def piece(q):
        return pl.ds(pl.multiple_of(c * HALF + q * PIECE, PIECE), PIECE)

    def c_f(p, q):
        return rcopy(xa.at[p, 0, piece(q)], xa.at[p, rF, piece(q)], sem_as.at[p, 0, q], sem_ar.at[p, 0, q], dev_f)

    def c_s(p, q):
        return rcopy(xa.at[p, 0, piece(q)], xa.at[p, rS, piece(q)], sem_as.at[p, 1, q], sem_ar.at[p, 1, q], dev_s)

    def c_d(p, q):
        return rcopy(xa.at[p, rF, piece(q)], xa.at[p, 3, piece(q)], sem_as.at[p, 2, q], sem_ar.at[p, 2, q], dev_s)

    def c_pair(p, r, q):
        return rcopy(xa.at[p, r, piece(q)], xa.at[p, r, piece(q)], sem_ds.at[p, r, q], sem_dr.at[p, r, q], partner)

    def rows_first(p, q):
        c_f(p, q).wait()
        c_d(p, q).start()
        c_pair(p, rF, q).start()

    def rows_second(p, q):
        c_s(p, q).wait()
        c_pair(p, rS, q).start()

    def rows_third(p, q):
        c_d(p, q).wait()
        c_pair(p, 3, q).start()

    def rows_done(p, r):
        for q in range(2):
            c_pair(p, r, q).wait()

    def own_first(q):
        rows = pl.ds(pl.multiple_of((1 - c) * HALF + q * PIECE, PIECE), PIECE)
        return rcopy(xa.at[c, 0, rows], xa.at[c, 0, rows], sem_os.at[q], sem_or.at[q], partner)

    own_second = rcopy(xa.at[c, 0, my_rows], xa.at[c, 0, my_rows], sem_os.at[2], sem_or.at[2], partner)

    x_load = pltpu.make_async_copy(x_hbm, xa.at[c, 0], sem_x)
    x_load.start()

    rtb[c * 4, 0:8, :] = ids_ref[...].astype(jnp.float32)
    rtb[c * 4, 8:16, :] = gate_ref[...]
    barrier = pltpu.get_barrier_semaphore()
    peers = [(r, flip) for r in range(4) for flip in (False, True) if (r, flip) != (0, False)]
    for r, flip in peers:
        pl.semaphore_signal(barrier, inc=1, device_id=dev(r, flip), device_id_type=MESH)
    pl.semaphore_wait(barrier, len(peers))

    def rt_link(r):
        b = c * 4 + r
        return rcopy(rtb.at[c * 4], rtb.at[b], sem_rs.at[r, 0], sem_rr.at[b], dev(r, False))

    def rt_pair(r):
        b = c * 4 + r
        return rcopy(rtb.at[b], rtb.at[b], sem_rs.at[r, 1], sem_rr.at[b], partner)

    for r in (3, 1, 2):
        rt_link(r).start()
    rt_pair(0).start()
    x_load.wait()
    for q in range(2):
        own_first(q).start()
    for q in range(2):
        @pl.when(c == 1)
        def _():
            own_first(q).wait_recv()

        c_f(0, q).start()
        c_s(0, q).start()
    for q in range(2):
        own_first(q).wait_send()
    own_second.start()
    for g in range(WSLOTS):
        for cp in w_copies(g):
            cp.start()

    t_row = lax.broadcasted_iota(jnp.int32, (ROWS, ROWS), 0)
    t_col = lax.broadcasted_iota(jnp.int32, (ROWS, ROWS), 1)
    utri[...] = jnp.where(t_row < t_col, 1.0, 0.0).astype(jnp.bfloat16)
    for r in (1, 2, 3):
        rt_link(r).wait()
        rt_pair(r).start()
    for r in range(4):
        rt_pair(r).wait_send()
        b = (1 - c) * 4 + r
        pltpu.make_async_copy(rtb.at[b], rtb.at[b], sem_rr.at[b]).wait()

    q_iota = lax.broadcasted_iota(jnp.int32, (CAP, ROWS), 0).astype(jnp.float32)

    def build(b, _):
        p = b // 4
        r = b % 4
        e_iota = (lax.broadcasted_iota(jnp.int32, (EL, ROWS), 0) + ep * EL).astype(jnp.float32)
        chosen = jnp.zeros((EL, ROWS), jnp.float32)
        gate = jnp.zeros((EL, ROWS), jnp.float32)
        for j in range(8):
            hit = rtb[b, j:j + 1, :] == e_iota
            chosen = jnp.where(hit, 1.0, chosen)
            gate = jnp.where(hit, rtb[b, 8 + j:9 + j, :], gate)
        rank = jnp.dot(chosen.astype(jnp.bfloat16), utri[...], preferred_element_type=jnp.float32)
        kk = jnp.where(chosen > 0.0, rank, -1.0)
        key[b] = kk
        hots = []
        for e in range(EL):
            hit = kk[e:e + 1, :] == q_iota
            hots.append(jnp.where(hit, 1.0, 0.0))
            gsum = jnp.sum(jnp.where(hit, gate[e:e + 1, :], 0.0), axis=1, keepdims=True)
            gp[p, e, pl.ds(pl.multiple_of(r * CAP, CAP), CAP), :] = jnp.broadcast_to(gsum, (CAP, 128))
        dt[b] = jnp.concatenate(hots, axis=0).T.astype(jnp.bfloat16)
        return 0

    lax.fori_loop(0, 8, build, 0)

    own_second.wait()

    @pl.when(c == 0)
    def _():
        for q in range(2):
            own_first(q).wait_recv()

    def dispatch_group(r, eg, put):
        kk = key.at[r]
        hots = [jnp.where(kk[pl.ds(eg * 4 + j, 1), :] == q_iota, 1.0, 0.0) for j in range(4)]
        hot = jnp.concatenate(hots, axis=0).astype(jnp.bfloat16)
        for n in range(4):
            res = jnp.dot(hot, xa[0, r, :, n * 512:(n + 1) * 512],
                          preferred_element_type=jnp.float32).astype(jnp.bfloat16)
            for j in range(4):
                for m in range(2):
                    put(j, n * 2 + m, r, res[j * CAP:(j + 1) * CAP, m * 256:(m + 1) * 256])

    def put_wdv(eg):
        def put(j, q, r, val):
            rows = pl.ds(pl.multiple_of((q % 2) * HALF + r * CAP, CAP), CAP)
            wdv[eg, j * 4 + q // 2, rows, :] = val
        return put

    def put_ob(j, q, r, val):
        rows = pl.ds(pl.multiple_of((q % 4) * HALF + r * CAP, CAP), CAP)
        ob[j * 2 + q // 4, rows, :] = val

    def put_xdp(j, q, r, val):
        xdp[j, pl.ds(pl.multiple_of(r * CAP, CAP), CAP), q * 256:(q + 1) * 256] = val

    def dispatch_block(r, _):
        @pl.when(r == 1)
        def _():
            rows_first(0, 0)
            rows_second(0, 0)
            rows_first(0, 1)
            c_s(1, 0).start()
            c_s(1, 1).start()
            rows_second(0, 1)
            rows_done(0, 1)
            rows_done(0, 2)

        for eg in range(2):
            dispatch_group(r, eg, put_wdv(eg))
        dispatch_group(r, 2, put_ob)
        dispatch_group(r, 3, put_xdp)
        return 0

    lax.fori_loop(0, 3, dispatch_block, 0)
    rows_third(0, 0)
    rows_third(0, 1)
    c_f(1, 0).start()
    c_f(1, 1).start()
    rows_done(0, 3)

    def expert(p, e, rows_of):
        g = p * EL + e
        for cp in w_copies(g):
            cp.wait()
        s = g % WSLOTS
        xe = rows_of()
        for n in range(2):
            cols = slice(n * 256, (n + 1) * 256)
            a = jnp.dot(xe, wgv[s, :, cols], preferred_element_type=jnp.float32)
            b = jnp.dot(xe, wuv[s, :, cols], preferred_element_type=jnp.float32)
            hb[p, e, :, cols] = (a * jax.nn.sigmoid(a) * b).astype(jnp.bfloat16)

        @pl.when(e + WSLOTS < EL)
        def _():
            for cp in w_copies(g + WSLOTS):
                cp.start()

    def dispatch(p, quad, blocks):
        for r in blocks:
            hots = [jnp.where(key[p * 4 + r, pl.ds(4 * quad + j, 1), :] == q_iota, 1.0, 0.0) for j in range(4)]
            hot = jnp.concatenate(hots, axis=0).astype(jnp.bfloat16)
            for n in range(4):
                cols = slice(n * 512, (n + 1) * 512)
                res = jnp.dot(hot, xa[p, r, :, cols], preferred_element_type=jnp.float32).astype(jnp.bfloat16)
                for j in range(4):
                    xdp[j, r * CAP:(r + 1) * CAP, cols] = res[j * CAP:(j + 1) * CAP]

    def group_wdv(eg, _):
        dispatch_group(3, eg, put_wdv(eg))

        def one(j, _):
            def rows_of():
                return jnp.concatenate([wdv[eg, j * 4 + q // 2, (q % 2) * HALF:(q % 2 + 1) * HALF, :]
                                        for q in range(8)], axis=1)
            expert(0, eg * 4 + j, rows_of)

            @pl.when((eg == 1) & (j == 1))
            def _():
                rows_first(1, 0)
                rows_second(1, 0)
            return 0

        lax.fori_loop(0, 4, one, 0)
        return 0

    def experts_ob(j, _):
        def rows_of():
            return jnp.concatenate([ob[j * 2 + q // 4, (q % 4) * HALF:(q % 4 + 1) * HALF, :]
                                    for q in range(8)], axis=1)
        expert(0, 8 + j, rows_of)
        return 0

    def experts_xdp(j, _):
        expert(0, 12 + j, lambda: xdp[j])

        @pl.when(j == 0)
        def _():
            rows_first(1, 1)
            rows_second(1, 1)
        return 0

    lax.fori_loop(0, 2, group_wdv, 0)
    wd_copy(0).start()
    dispatch_group(3, 2, put_ob)
    lax.fori_loop(0, 4, experts_ob, 0)
    dispatch_group(3, 3, put_xdp)
    lax.fori_loop(0, 4, experts_xdp, 0)
    for g in range(WSLOTS):
        if g == 2:
            wd_copy(1).start()
        for cp in w_copies(EL + g):
            cp.start()

    def k_pair(u):
        s = u % 2
        return rcopy(ps, dr.at[s], sem_ps, sem_pr.at[s], partner)

    def k_first(u, which):
        s = u % SLOTS
        src = pm.at[s, 3] if which == 0 else pm.at[s, rF]
        return rcopy(src, rf.at[s, which], sem_fs.at[s, which], sem_fr.at[s, which], dev_f)

    def k_second(u):
        s = u % SLOTS
        return rcopy(pm.at[s, rS], rs.at[s], sem_ss.at[s], sem_sr.at[s], dev_s)

    def k_out(u):
        k = u % NCH
        cols = pl.ds(pl.multiple_of(k * CH, CH), CH)
        return rcopy(yst.at[u % SLOTS], y_hbm.at[my_rows, cols], sem_ys.at[k], sem_yr.at[k], partner)

    def k_local(u):
        k = u % NCH
        cols = pl.ds(pl.multiple_of(k * CH, CH), CH)
        return pltpu.make_async_copy(yst.at[u % SLOTS], y_hbm.at[my_rows, cols], sem_yl.at[k])

    def out_drain(u):
        @pl.when(c == u // NCH)
        def _():
            k_local(u).wait()

        @pl.when(c != u // NCH)
        def _():
            k_out(u).wait_send()

    def stage1(u):
        k_pair(u).wait()
        s = u % SLOTS
        for r in (3, 1, 2, 0):
            pm[s, r] = pm[s, r] + dr[u % 2, r]
        k_first(u, 0).start()
        k_first(u, 1).start()

    def stage2(u):
        s = u % SLOTS
        k_first(u, 0).wait()
        pm[s, rS] = pm[s, rS] + rf[s, 0]
        k_second(u).start()
        k_first(u, 1).wait()
        pm[s, 0] = pm[s, 0] + rf[s, 1]

    def stage3(u):
        s = u % SLOTS
        k_second(u).wait()

        @pl.when(u >= SLOTS)
        def _():
            out_drain(u - SLOTS)

        yst[s] = (pm[s, 0] + rs[s]).astype(jnp.bfloat16)

        @pl.when(c == u // NCH)
        def _():
            k_local(u).start()

        @pl.when(c != u // NCH)
        def _():
            k_out(u).start()

    def compute(u):
        p = u // NCH
        s2 = u % 2
        s4 = u % SLOTS
        wd_copy(u).wait()

        for e in range(EL):
            o = jnp.dot(hb[p, e], wdv[s2, e], preferred_element_type=jnp.float32)
            g = gp[p, e]
            o = o * jnp.concatenate([g, g], axis=1)
            hi = o.astype(jnp.bfloat16)
            rest = o - hi.astype(jnp.float32)
            mid = rest.astype(jnp.bfloat16)
            lo = (rest - mid.astype(jnp.float32)).astype(jnp.bfloat16)
            rows = slice(e * CAP, (e + 1) * CAP)
            for r in range(4):
                part = slice(r * CAP, (r + 1) * CAP)
                ob[r, rows, :] = hi[part]
                ob[4 + r, rows, :] = mid[part]
                ob[8 + r, rows, :] = lo[part]

        @pl.when(u + 2 < UNITS)
        def _():
            wd_copy(u + 2).start()

        @pl.when(u == 1)
        def _():
            stage1(0)

        @pl.when(u >= 2)
        def _():
            stage2(u - 2)

        def combine(rows, store):
            for r in range(4):
                sel = dt[p * 4 + r, rows, :]
                acc = jnp.dot(sel, ob[r], preferred_element_type=jnp.float32)
                acc += jnp.dot(sel, ob[4 + r], preferred_element_type=jnp.float32)
                acc += jnp.dot(sel, ob[8 + r], preferred_element_type=jnp.float32)
                store(r, acc)

        def store_other(r, acc):
            ps[r] = acc

        def store_mine(r, acc):
            pm[s4, r] = acc

        combine(other_rows, store_other)
        k_pair(u).start()
        combine(my_rows, store_mine)

    def unit(i, _):
        @pl.when(i >= 4)
        def _():
            stage3(i - 4)

        @pl.when(i == NCH)
        def _():
            for j in (2, 3):
                expert(1, EL - 4 + j, lambda: xdp[j])

        @pl.when(i < UNITS)
        def _():
            compute(i)

        first = 2 * (i - 1)
        beside = (i >= 1) & (i < NCH)

        @pl.when(i == 1)
        def _():
            rows_third(1, 0)
            rows_third(1, 1)

        @pl.when(beside & (i % 2 == 1))
        def _():
            dispatch(1, i // 2, (0, 1, 2))
            stage1(i)

        @pl.when(i == 1)
        def _():
            rows_done(1, 3)

        @pl.when(beside & (i % 2 == 1))
        def _():
            dispatch(1, i // 2, (3,))

        @pl.when(beside)
        def _():
            expert(1, first, lambda: xdp[first % 4])

        @pl.when((i >= UNITS) & (i < UNITS + 2))
        def _():
            stage2(i - 2)

        @pl.when((i < UNITS) & (i > 0) & ((i >= NCH) | (i % 2 == 0)))
        def _():
            stage1(i)

        @pl.when(beside)
        def _():
            expert(1, first + 1, lambda: xdp[first % 4 + 1])
        return 0

    rows_done(1, 1)
    rows_done(1, 2)
    lax.fori_loop(0, UNITS + 4, unit, 0)

    for u in range(UNITS - SLOTS, UNITS):
        out_drain(u)
    for k in range(NCH):
        k_out(k).wait_recv()


def solution(mesh):
    row_spec = P(('dp', 'ep', 'tp'), None)
    bf, f32 = jnp.bfloat16, jnp.float32

    def local_moe(x, ids, gate, wg, wu, wd):
        anyspec = pl.BlockSpec(memory_space=pl.ANY)
        dma = pltpu.SemaphoreType.DMA
        return pl.pallas_call(
            moe_kernel,
            out_shape=jax.ShapeDtypeStruct((ROWS, DM), bf),
            in_specs=[pl.BlockSpec(memory_space=pltpu.VMEM)] * 2 + [anyspec] * 4,
            out_specs=anyspec,
            scratch_shapes=[
                pltpu.VMEM((2, 4, ROWS, DM), bf),
                pltpu.VMEM((8, 16, ROWS), f32),
                pltpu.VMEM((8, EL, ROWS), f32),
                pltpu.VMEM((8, ROWS, EL * CAP), bf),
                pltpu.VMEM((2, EL, 4 * CAP, 128), f32),
                pltpu.VMEM((ROWS, ROWS), bf),
                pltpu.VMEM((4, 4 * CAP, DM), bf),
                pltpu.VMEM((2, EL, 4 * CAP, FF), bf),
                pltpu.VMEM((WSLOTS, DM, FF), bf),
                pltpu.VMEM((WSLOTS, DM, FF), bf),
                pltpu.VMEM((2, EL, FF, CH), bf),
                pltpu.VMEM((12, EL * CAP, CH), bf),
                pltpu.VMEM((SLOTS, 4, HALF, CH), f32),
                pltpu.VMEM((4, HALF, CH), f32),
                pltpu.VMEM((2, 4, HALF, CH), f32),
                pltpu.VMEM((SLOTS, 2, HALF, CH), f32),
                pltpu.VMEM((SLOTS, HALF, CH), f32),
                pltpu.VMEM((SLOTS, HALF, CH), bf),
                dma, dma((WSLOTS, 2)), dma((2,)), dma((4, 2)), dma((8,)), dma((3,)), dma((3,)),
                dma((2, 3, 2)), dma((2, 3, 2)), dma((2, 4, 2)), dma((2, 4, 2)), dma, dma((2,)),
                dma((SLOTS, 2)), dma((SLOTS, 2)), dma((SLOTS,)), dma((SLOTS,)), dma((NCH,)), dma((NCH,)), dma((NCH,)),
            ],
            compiler_params=pltpu.CompilerParams(
                collective_id=0, has_side_effects=True, vmem_limit_bytes=67_043_328),
        )(ids.T, gate.T, x, wg, wu, wd)

    return jax.shard_map(
        local_moe, mesh=mesh,
        in_specs=(row_spec, row_spec, row_spec, P('ep', None, 'tp'), P('ep', None, 'tp'), P('ep', 'tp', None)),
        out_specs=row_spec, check_vma=False)
```

```python
import functools

import jax
import jax.numpy as jnp
from jax import lax
from jax.experimental import pallas as pl
from jax.experimental.pallas import tpu as pltpu
from jax.sharding import PartitionSpec as P

MESH = pl.DeviceIdType.MESH
ROWS = 384
HALF = 192
PIECE = 96
CAP = 48
DM = 2048
FF = 512
EL = 16
CH = 256
NCH = DM // CH
UNITS = 2 * NCH
WSLOTS = 3
SLOTS = 4


def moe_kernel(ids_ref, gate_ref, x_hbm, wg_hbm, wu_hbm, wd_hbm, y_hbm,
               xa, rtb, key, dt, gp, utri, xdp, hb, wgv, wuv, wdv, ob,
               pm, ps, dr, rf, rs, yst,
               sem_x, sem_w, sem_wd, sem_rs, sem_rr, sem_os, sem_or,
               sem_as, sem_ar, sem_ds, sem_dr, sem_ps, sem_pr, sem_fs, sem_fr,
               sem_ss, sem_sr, sem_ys, sem_yr, sem_yl):
    ep = lax.axis_index('ep')
    ty = lax.axis_index('tp')
    cx = ep // 2
    c = ep % 2
    rF = 1 + c
    rS = 2 - c
    my_rows = pl.ds(pl.multiple_of(c * HALF, HALF), HALF)
    other_rows = pl.ds(pl.multiple_of((1 - c) * HALF, HALF), HALF)

    def dev(r, flip):
        nx = 1 - cx if r & 1 else cx
        nc = 1 - c if flip else c
        ny = 1 - ty if r & 2 else ty
        return {'ep': nx * 2 + nc, 'tp': ny}

    partner = dev(0, True)
    dev_f = {'ep': (cx * c + (1 - cx) * (1 - c)) * 2 + c, 'tp': ty * (1 - c) + (1 - ty) * c}
    dev_s = {'ep': (cx * (1 - c) + (1 - cx) * c) * 2 + c, 'tp': ty * c + (1 - ty) * (1 - c)}

    def rcopy(src, dst, ssem, rsem, device):
        return pltpu.make_async_remote_copy(src_ref=src, dst_ref=dst, send_sem=ssem, recv_sem=rsem,
                                            device_id=device, device_id_type=MESH)

    def w_copies(g):
        e = g % EL
        s = g % WSLOTS
        return (pltpu.make_async_copy(wg_hbm.at[e], wgv.at[s], sem_w.at[s, 0]),
                pltpu.make_async_copy(wu_hbm.at[e], wuv.at[s], sem_w.at[s, 1]))

    def wd_copy(u):
        col = pl.ds(pl.multiple_of((u % NCH) * CH, CH), CH)
        return pltpu.make_async_copy(wd_hbm.at[:, :, col], wdv.at[u % 2], sem_wd.at[u % 2])

    def piece(q):
        return pl.ds(pl.multiple_of(c * HALF + q * PIECE, PIECE), PIECE)

    def c_f(p, q):
        return rcopy(xa.at[p, 0, piece(q)], xa.at[p, rF, piece(q)], sem_as.at[p, 0, q], sem_ar.at[p, 0, q], dev_f)

    def c_s(p, q):
        return rcopy(xa.at[p, 0, piece(q)], xa.at[p, rS, piece(q)], sem_as.at[p, 1, q], sem_ar.at[p, 1, q], dev_s)

    def c_d(p, q):
        return rcopy(xa.at[p, rF, piece(q)], xa.at[p, 3, piece(q)], sem_as.at[p, 2, q], sem_ar.at[p, 2, q], dev_s)

    def c_pair(p, r, q):
        return rcopy(xa.at[p, r, piece(q)], xa.at[p, r, piece(q)], sem_ds.at[p, r, q], sem_dr.at[p, r, q], partner)

    def rows_first(p, q):
        c_f(p, q).wait()
        c_d(p, q).start()
        c_pair(p, rF, q).start()

    def rows_second(p, q):
        c_s(p, q).wait()
        c_pair(p, rS, q).start()

    def rows_third(p, q):
        c_d(p, q).wait()
        c_pair(p, 3, q).start()

    def rows_done(p, r):
        for q in range(2):
            c_pair(p, r, q).wait()

    def own_first(q):
        rows = pl.ds(pl.multiple_of((1 - c) * HALF + q * PIECE, PIECE), PIECE)
        return rcopy(xa.at[c, 0, rows], xa.at[c, 0, rows], sem_os.at[q], sem_or.at[q], partner)

    own_second = rcopy(xa.at[c, 0, my_rows], xa.at[c, 0, my_rows], sem_os.at[2], sem_or.at[2], partner)

    x_load = pltpu.make_async_copy(x_hbm, xa.at[c, 0], sem_x)
    x_load.start()

    rtb[c * 4, 0:8, :] = ids_ref[...].astype(jnp.float32)
    rtb[c * 4, 8:16, :] = gate_ref[...]
    barrier = pltpu.get_barrier_semaphore()
    peers = [(r, flip) for r in range(4) for flip in (False, True) if (r, flip) != (0, False)]
    for r, flip in peers:
        pl.semaphore_signal(barrier, inc=1, device_id=dev(r, flip), device_id_type=MESH)
    pl.semaphore_wait(barrier, len(peers))

    def rt_link(r):
        b = c * 4 + r
        return rcopy(rtb.at[c * 4], rtb.at[b], sem_rs.at[r, 0], sem_rr.at[b], dev(r, False))

    def rt_pair(r):
        b = c * 4 + r
        return rcopy(rtb.at[b], rtb.at[b], sem_rs.at[r, 1], sem_rr.at[b], partner)

    for r in (3, 1, 2):
        rt_link(r).start()
    rt_pair(0).start()
    x_load.wait()
    for q in range(2):
        own_first(q).start()
    for q in range(2):
        @pl.when(c == 1)
        def _():
            own_first(q).wait_recv()

        c_f(0, q).start()
        c_s(0, q).start()
    for q in range(2):
        own_first(q).wait_send()
    own_second.start()
    for g in range(WSLOTS):
        for cp in w_copies(g):
            cp.start()

    t_row = lax.broadcasted_iota(jnp.int32, (ROWS, ROWS), 0)
    t_col = lax.broadcasted_iota(jnp.int32, (ROWS, ROWS), 1)
    utri[...] = jnp.where(t_row < t_col, 1.0, 0.0).astype(jnp.bfloat16)
    for r in (1, 2, 3):
        rt_link(r).wait()
        rt_pair(r).start()
    for r in range(4):
        rt_pair(r).wait_send()
        b = (1 - c) * 4 + r
        pltpu.make_async_copy(rtb.at[b], rtb.at[b], sem_rr.at[b]).wait()

    q_iota = lax.broadcasted_iota(jnp.int32, (CAP, ROWS), 0).astype(jnp.float32)

    def build(b, _):
        p = b // 4
        r = b % 4
        e_iota = (lax.broadcasted_iota(jnp.int32, (EL, ROWS), 0) + ep * EL).astype(jnp.float32)
        chosen = jnp.zeros((EL, ROWS), jnp.float32)
        gate = jnp.zeros((EL, ROWS), jnp.float32)
        for j in range(8):
            hit = rtb[b, j:j + 1, :] == e_iota
            chosen = jnp.where(hit, 1.0, chosen)
            gate = jnp.where(hit, rtb[b, 8 + j:9 + j, :], gate)
        rank = jnp.dot(chosen.astype(jnp.bfloat16), utri[...], preferred_element_type=jnp.float32)
        kk = jnp.where(chosen > 0.0, rank, -1.0)
        key[b] = kk
        hots = []
        for e in range(EL):
            hit = kk[e:e + 1, :] == q_iota
            hots.append(jnp.where(hit, 1.0, 0.0))
            gsum = jnp.sum(jnp.where(hit, gate[e:e + 1, :], 0.0), axis=1, keepdims=True)
            gp[p, e, pl.ds(pl.multiple_of(r * CAP, CAP), CAP), :] = jnp.broadcast_to(gsum, (CAP, 128))
        dt[b] = jnp.concatenate(hots, axis=0).T.astype(jnp.bfloat16)
        return 0

    lax.fori_loop(0, 8, build, 0)

    own_second.wait()

    @pl.when(c == 0)
    def _():
        for q in range(2):
            own_first(q).wait_recv()

    def dispatch_group(r, eg, put):
        kk = key.at[r]
        hots = [jnp.where(kk[pl.ds(eg * 4 + j, 1), :] == q_iota, 1.0, 0.0) for j in range(4)]
        hot = jnp.concatenate(hots, axis=0).astype(jnp.bfloat16)
        for n in range(4):
            res = jnp.dot(hot, xa[0, r, :, n * 512:(n + 1) * 512],
                          preferred_element_type=jnp.float32).astype(jnp.bfloat16)
            for j in range(4):
                for m in range(2):
                    put(j, n * 2 + m, r, res[j * CAP:(j + 1) * CAP, m * 256:(m + 1) * 256])

    def put_wdv(eg):
        def put(j, q, r, val):
            rows = pl.ds(pl.multiple_of((q % 2) * HALF + r * CAP, CAP), CAP)
            wdv[eg, j * 4 + q // 2, rows, :] = val
        return put

    def put_ob(j, q, r, val):
        rows = pl.ds(pl.multiple_of((q % 4) * HALF + r * CAP, CAP), CAP)
        ob[j * 2 + q // 4, rows, :] = val

    def put_xdp(j, q, r, val):
        xdp[j, pl.ds(pl.multiple_of(r * CAP, CAP), CAP), q * 256:(q + 1) * 256] = val

    def dispatch_block(r, _):
        @pl.when(r == 1)
        def _():
            rows_first(0, 0)
            rows_second(0, 0)
            rows_first(0, 1)
            c_s(1, 0).start()
            c_s(1, 1).start()
            rows_second(0, 1)
            rows_done(0, 1)
            rows_done(0, 2)

        for eg in range(2):
            dispatch_group(r, eg, put_wdv(eg))
        dispatch_group(r, 2, put_ob)
        dispatch_group(r, 3, put_xdp)
        return 0

    lax.fori_loop(0, 3, dispatch_block, 0)
    rows_third(0, 0)
    rows_third(0, 1)
    c_f(1, 0).start()
    c_f(1, 1).start()
    rows_done(0, 3)

    def expert(p, e, rows_of):
        g = p * EL + e
        for cp in w_copies(g):
            cp.wait()
        s = g % WSLOTS
        xe = rows_of()
        for n in range(2):
            cols = slice(n * 256, (n + 1) * 256)
            a = jnp.dot(xe, wgv[s, :, cols], preferred_element_type=jnp.float32)
            b = jnp.dot(xe, wuv[s, :, cols], preferred_element_type=jnp.float32)
            hb[p, e, :, cols] = (a * jax.nn.sigmoid(a) * b).astype(jnp.bfloat16)

        @pl.when(e + WSLOTS < EL)
        def _():
            for cp in w_copies(g + WSLOTS):
                cp.start()

    def dispatch(p, quad, blocks):
        for r in blocks:
            hots = [jnp.where(key[p * 4 + r, pl.ds(4 * quad + j, 1), :] == q_iota, 1.0, 0.0) for j in range(4)]
            hot = jnp.concatenate(hots, axis=0).astype(jnp.bfloat16)
            for n in range(4):
                cols = slice(n * 512, (n + 1) * 512)
                res = jnp.dot(hot, xa[p, r, :, cols], preferred_element_type=jnp.float32).astype(jnp.bfloat16)
                for j in range(4):
                    xdp[j, r * CAP:(r + 1) * CAP, cols] = res[j * CAP:(j + 1) * CAP]

    def group_wdv(eg, _):
        dispatch_group(3, eg, put_wdv(eg))

        def one(j, _):
            def rows_of():
                return jnp.concatenate([wdv[eg, j * 4 + q // 2, (q % 2) * HALF:(q % 2 + 1) * HALF, :]
                                        for q in range(8)], axis=1)
            expert(0, eg * 4 + j, rows_of)

            @pl.when((eg == 1) & (j == 1))
            def _():
                rows_first(1, 0)
                rows_second(1, 0)
            return 0

        lax.fori_loop(0, 4, one, 0)
        return 0

    def experts_ob(j, _):
        def rows_of():
            return jnp.concatenate([ob[j * 2 + q // 4, (q % 4) * HALF:(q % 4 + 1) * HALF, :]
                                    for q in range(8)], axis=1)
        expert(0, 8 + j, rows_of)
        return 0

    def experts_xdp(j, _):
        expert(0, 12 + j, lambda: xdp[j])

        @pl.when(j == 0)
        def _():
            rows_first(1, 1)
            rows_second(1, 1)
        return 0

    lax.fori_loop(0, 2, group_wdv, 0)
    wd_copy(0).start()
    dispatch_group(3, 2, put_ob)
    lax.fori_loop(0, 4, experts_ob, 0)
    dispatch_group(3, 3, put_xdp)
    lax.fori_loop(0, 4, experts_xdp, 0)
    for g in range(WSLOTS):
        if g == 2:
            wd_copy(1).start()
        for cp in w_copies(EL + g):
            cp.start()

    def k_pair(u):
        s = u % 2
        return rcopy(ps, dr.at[s], sem_ps, sem_pr.at[s], partner)

    def k_first(u, which):
        s = u % SLOTS
        src = pm.at[s, 3] if which == 0 else pm.at[s, rF]
        return rcopy(src, rf.at[s, which], sem_fs.at[s, which], sem_fr.at[s, which], dev_f)

    def k_second(u):
        s = u % SLOTS
        return rcopy(pm.at[s, rS], rs.at[s], sem_ss.at[s], sem_sr.at[s], dev_s)

    def k_out(u):
        k = u % NCH
        cols = pl.ds(pl.multiple_of(k * CH, CH), CH)
        return rcopy(yst.at[u % SLOTS], y_hbm.at[my_rows, cols], sem_ys.at[k], sem_yr.at[k], partner)

    def k_local(u):
        k = u % NCH
        cols = pl.ds(pl.multiple_of(k * CH, CH), CH)
        return pltpu.make_async_copy(yst.at[u % SLOTS], y_hbm.at[my_rows, cols], sem_yl.at[k])

    def out_drain(u):
        @pl.when(c == u // NCH)
        def _():
            k_local(u).wait()

        @pl.when(c != u // NCH)
        def _():
            k_out(u).wait_send()

    def stage1(u):
        k_pair(u).wait()
        s = u % SLOTS
        pm[s, 3] = pm[s, 3] + dr[u % 2, 3]
        k_first(u, 0).start()
        pm[s, rF] = pm[s, rF] + dr[u % 2, rF]
        k_first(u, 1).start()
        pm[s, rS] = pm[s, rS] + dr[u % 2, rS]
        pm[s, 0] = pm[s, 0] + dr[u % 2, 0]

    def stage2(u):
        s = u % SLOTS
        k_first(u, 0).wait()
        pm[s, rS] = pm[s, rS] + rf[s, 0]
        k_second(u).start()
        k_first(u, 1).wait()
        pm[s, 0] = pm[s, 0] + rf[s, 1]

    def stage3(u):
        s = u % SLOTS
        k_second(u).wait()

        @pl.when(u >= SLOTS)
        def _():
            out_drain(u - SLOTS)

        yst[s] = (pm[s, 0] + rs[s]).astype(jnp.bfloat16)

        @pl.when(c == u // NCH)
        def _():
            k_local(u).start()

        @pl.when(c != u // NCH)
        def _():
            k_out(u).start()

    def compute(u):
        p = u // NCH
        s2 = u % 2
        s4 = u % SLOTS
        wd_copy(u).wait()

        for e in range(EL):
            o = jnp.dot(hb[p, e], wdv[s2, e], preferred_element_type=jnp.float32)
            g = gp[p, e]
            o = o * jnp.concatenate([g, g], axis=1)
            hi = o.astype(jnp.bfloat16)
            rest = o - hi.astype(jnp.float32)
            mid = rest.astype(jnp.bfloat16)
            lo = (rest - mid.astype(jnp.float32)).astype(jnp.bfloat16)
            rows = slice(e * CAP, (e + 1) * CAP)
            for r in range(4):
                part = slice(r * CAP, (r + 1) * CAP)
                ob[r, rows, :] = hi[part]
                ob[4 + r, rows, :] = mid[part]
                ob[8 + r, rows, :] = lo[part]

        @pl.when(u + 2 < UNITS)
        def _():
            wd_copy(u + 2).start()

        @pl.when(u == 1)
        def _():
            stage1(0)

        def combine(rows, store):
            for r in range(4):
                sel = dt[p * 4 + r, rows, :]
                acc = jnp.dot(sel, ob[r], preferred_element_type=jnp.float32)
                acc += jnp.dot(sel, ob[4 + r], preferred_element_type=jnp.float32)
                acc += jnp.dot(sel, ob[8 + r], preferred_element_type=jnp.float32)
                store(r, acc)

        def store_other(r, acc):
            ps[r] = acc

        def store_mine(r, acc):
            pm[s4, r] = acc

        combine(other_rows, store_other)
        k_pair(u).start()

        @pl.when(u >= 2)
        def _():
            stage2(u - 2)

        combine(my_rows, store_mine)

    def unit(i, _):
        @pl.when(i >= 4)
        def _():
            stage3(i - 4)

        @pl.when(i == NCH)
        def _():
            for j in (2, 3):
                expert(1, EL - 4 + j, lambda: xdp[j])

        @pl.when(i < UNITS)
        def _():
            compute(i)

        first = 2 * (i - 1)
        beside = (i >= 1) & (i < NCH)

        @pl.when(i == 1)
        def _():
            rows_third(1, 0)
            rows_third(1, 1)

        @pl.when(beside & (i % 2 == 1))
        def _():
            dispatch(1, i // 2, (0, 1, 2))
            stage1(i)

        @pl.when(i == 1)
        def _():
            rows_done(1, 3)

        @pl.when(beside & (i % 2 == 1))
        def _():
            dispatch(1, i // 2, (3,))

        @pl.when(beside)
        def _():
            expert(1, first, lambda: xdp[first % 4])

        @pl.when((i >= UNITS) & (i < UNITS + 2))
        def _():
            stage2(i - 2)

        @pl.when((i < UNITS) & (i > 0) & ((i >= NCH) | (i % 2 == 0)))
        def _():
            stage1(i)

        @pl.when(beside)
        def _():
            expert(1, first + 1, lambda: xdp[first % 4 + 1])
        return 0

    rows_done(1, 1)
    rows_done(1, 2)
    lax.fori_loop(0, UNITS + 4, unit, 0)

    for u in range(UNITS - SLOTS, UNITS):
        out_drain(u)
    for k in range(NCH):
        k_out(k).wait_recv()


def solution(mesh):
    row_spec = P(('dp', 'ep', 'tp'), None)
    bf, f32 = jnp.bfloat16, jnp.float32

    def local_moe(x, ids, gate, wg, wu, wd):
        anyspec = pl.BlockSpec(memory_space=pl.ANY)
        dma = pltpu.SemaphoreType.DMA
        return pl.pallas_call(
            moe_kernel,
            out_shape=jax.ShapeDtypeStruct((ROWS, DM), bf),
            in_specs=[pl.BlockSpec(memory_space=pltpu.VMEM)] * 2 + [anyspec] * 4,
            out_specs=anyspec,
            scratch_shapes=[
                pltpu.VMEM((2, 4, ROWS, DM), bf),
                pltpu.VMEM((8, 16, ROWS), f32),
                pltpu.VMEM((8, EL, ROWS), f32),
                pltpu.VMEM((8, ROWS, EL * CAP), bf),
                pltpu.VMEM((2, EL, 4 * CAP, 128), f32),
                pltpu.VMEM((ROWS, ROWS), bf),
                pltpu.VMEM((4, 4 * CAP, DM), bf),
                pltpu.VMEM((2, EL, 4 * CAP, FF), bf),
                pltpu.VMEM((WSLOTS, DM, FF), bf),
                pltpu.VMEM((WSLOTS, DM, FF), bf),
                pltpu.VMEM((2, EL, FF, CH), bf),
                pltpu.VMEM((12, EL * CAP, CH), bf),
                pltpu.VMEM((SLOTS, 4, HALF, CH), f32),
                pltpu.VMEM((4, HALF, CH), f32),
                pltpu.VMEM((2, 4, HALF, CH), f32),
                pltpu.VMEM((SLOTS, 2, HALF, CH), f32),
                pltpu.VMEM((SLOTS, HALF, CH), f32),
                pltpu.VMEM((SLOTS, HALF, CH), bf),
                dma, dma((WSLOTS, 2)), dma((2,)), dma((4, 2)), dma((8,)), dma((3,)), dma((3,)),
                dma((2, 3, 2)), dma((2, 3, 2)), dma((2, 4, 2)), dma((2, 4, 2)), dma, dma((2,)),
                dma((SLOTS, 2)), dma((SLOTS, 2)), dma((SLOTS,)), dma((SLOTS,)), dma((NCH,)), dma((NCH,)), dma((NCH,)),
            ],
            compiler_params=pltpu.CompilerParams(
                collective_id=0, has_side_effects=True, vmem_limit_bytes=67_043_328),
        )(ids.T, gate.T, x, wg, wu, wd)

    return jax.shard_map(
        local_moe, mesh=mesh,
        in_specs=(row_spec, row_spec, row_spec, P('ep', None, 'tp'), P('ep', None, 'tp'), P('ep', 'tp', None)),
        out_specs=row_spec, check_vma=False)
```
